128 devices in a mesh: dp: 8 (over x, z_hi), cls: 16 (over z_lo, y, core).
Axes of the slice: x: 4, y: 4, z: 4 (z_hi: 2, z_lo: 2; z = z_hi * 2 + z_lo), core: 2. Of those that a mesh axis runs over, the one named last changes fastest.
Arguments:
- sketches: bfloat16 [32768, 4096], P(('dp', 'cls')), may hold values from -6 to 6
- labels: int32 [32768], P(('dp', 'cls')), may hold values from 0 to 15, as said below
- places: int32 [32768], P(('dp', 'cls')), may hold values from 0 to 4095, as said below
- counts: int32 [16, 8, 128], P('cls'), may hold values from 0 to 4, as said below
- chosen: int32 [3, 16], P(None, 'cls'), may hold values from 0 to 4095, as said below
Outputs:
- gain_scores: float32 [3, 16, 4096], P(None, 'cls', 'dp')
- coverage: float32 [16, 4096], P('cls', 'dp')
The draws below stay inside these ranges and needn't reach their ends.
Inputs may be any that keep to these rules, and one draw needn't show every extreme that they name: `labels`: every class has 8 or more examples. `places`: an example of device s (its index along dp and cls together) with class k has place m * 512 + s * 4 + j in class k's block: m is the member of dp that receives it, and for each k, m and s the j run over 0 to counts[k, m, s] - 1 without gaps, so no two examples share a place. In every draw one class and member receive 4 examples from every device. counts[k, m, s] is the number of examples of device s that take places of class k on member m. chosen[t, k] is a place of class k's block that holds an example; the 3 picks of a class differ.
All inputs are finite; a program needn't handle non-finite values.
Results may differ from the reference program's by a relative error of at most 0.0003.
Values may be sent and summed in bfloat16 or wider, within the bound.
A program may use at most 128 MiB of HBM per device.

```python
import jax
import jax.numpy as jnp
from jax import lax

D = 4096
ROW_DEV = 256
STEPS = 3
CLASSES = 16
SUB = 4
CAP = 512
BLOCK = 4096
ROWS = 32768
N_DP = 8
DEVICES = 128


def layout_tables(key):
    slot_count = 2 * ROW_DEV
    class_key, full_key, member_key, base_key, pick_key = jax.random.split(jax.random.fold_in(key, 7), 5)
    class_level = jax.random.randint(class_key, (CLASSES,), 0, 3)
    full_class = jax.random.randint(full_key, (), 0, CLASSES)
    full_member = jax.random.randint(member_key, (), 0, N_DP)
    item_index = jnp.arange(slot_count, dtype=jnp.int32)
    item_member = item_index // (CLASSES * SUB)
    item_class = item_index // SUB % CLASSES
    item_place = item_index % SUB
    source = jnp.arange(DEVICES, dtype=jnp.int32)[:, None]
    promised = (item_class[None, :] == source % CLASSES) & (item_member[None, :] == source // CLASSES % N_DP) & (item_place[None, :] == 0)
    full_item = (item_class == full_class) & (item_member == full_member)
    base = jax.random.randint(base_key, (DEVICES, slot_count), 0, 2 ** 16)
    level = base + class_level[item_class][None, :] * 2 ** 16 + promised.astype(jnp.int32) * 2 ** 18 + full_item.astype(jnp.int32)[None, :] * 2 ** 19
    score = level * slot_count + item_index[None, :]
    top_scores, picked_items = lax.top_k(score, ROW_DEV)
    group = picked_items // SUB
    same_group = group[:, :, None] == group[:, None, :]
    earlier = picked_items[:, None, :] < picked_items[:, :, None]
    rank = jnp.sum((same_group & earlier).astype(jnp.int32), axis=2)
    member = group // CLASSES
    klass = group % CLASSES
    places = member * CAP + source * SUB + rank
    group_hits = (group[:, :, None] == jnp.arange(N_DP * CLASSES, dtype=jnp.int32)[None, None, :]).astype(jnp.int32)
    per_group = jnp.sum(group_hits, axis=1).reshape(DEVICES, N_DP, CLASSES)
    counts = jnp.transpose(per_group, (2, 1, 0))
    valid = (jnp.arange(SUB, dtype=jnp.int32)[None, None, None, :] < counts[:, :, :, None]).reshape(CLASSES, BLOCK)
    noise = jax.random.randint(pick_key, (CLASSES, BLOCK), 0, 256)
    pick_score = (noise + valid.astype(jnp.int32) * 512) * BLOCK + jnp.arange(BLOCK, dtype=jnp.int32)[None, :]
    top_picks, pick_places = lax.top_k(pick_score, STEPS)
    return (klass.reshape(-1), places.reshape(-1), counts, jnp.transpose(pick_places))


def draw_labels(key, part):
    return layout_tables(key)[0].astype(jnp.int32)


def draw_places(key, part):
    return layout_tables(key)[1].astype(jnp.int32)


def draw_counts(key, part):
    return layout_tables(key)[2].astype(jnp.int32)


def draw_chosen(key, part):
    return layout_tables(key)[3].astype(jnp.int32)


def draw_sketches(key, part):
    labels = layout_tables(key)[0].astype(jnp.int32)
    mean_key, noise_key, scale_key = jax.random.split(jax.random.fold_in(key, 11), 3)
    class_means = jnp.clip(jax.random.normal(mean_key, (CLASSES, D), jnp.float32), -4.2, 4.2)
    centers = 0.6 * class_means[labels]
    noise = jnp.clip(jax.random.normal(noise_key, (ROWS, D), jnp.float32), -4.2, 4.2)
    raw = centers + noise
    row_rms = jnp.sqrt(jnp.mean(raw * raw, axis=1, keepdims=True))
    scale = jnp.exp(jax.random.uniform(scale_key, (ROWS, 1), jnp.float32, jnp.log(0.98), jnp.log(1.02)))
    values = jnp.clip(scale * raw / row_rms, -6.0, 6.0)
    return values.astype(jnp.bfloat16)


def setup_inputs(seed: int = 0) -> dict:
    seeds = jax.random.split(jax.random.key(seed), 6)
    sketches = draw_sketches(jax.random.fold_in(seeds[5], 71), 0)
    labels = draw_labels(jax.random.fold_in(seeds[5], 71), 0)
    places = draw_places(jax.random.fold_in(seeds[5], 71), 0)
    counts = draw_counts(jax.random.fold_in(seeds[5], 71), 0)
    chosen = draw_chosen(jax.random.fold_in(seeds[5], 71), 0)
    return {"sketches": sketches, "labels": labels, "places": places, "counts": counts, "chosen": chosen}


def class_scores(class_block, class_counts, class_picks):
    wide = class_block.astype(jnp.float32)
    norms = jnp.sum(wide * wide, axis=1)
    inner = jnp.dot(class_block, class_block.T, preferred_element_type=jnp.float32)
    spread = (norms[:, None] + norms[None, :] - 2.0 * inner) / D
    valid = (jnp.arange(SUB, dtype=jnp.int32)[None, None, :] < class_counts[:, :, None]).reshape(-1)
    weight = valid.astype(jnp.float32)
    bound = jnp.max(jnp.where(valid[:, None] & valid[None, :], spread, 0.0))
    similar = bound - spread
    total = jnp.sum(class_counts).astype(jnp.float32)
    cover = jnp.zeros((similar.shape[0],), jnp.float32)
    scores = []
    for turn_index in range(STEPS):
        scores.append(jnp.sum(weight[:, None] * jnp.maximum(similar - cover[:, None], 0.0), axis=0) * weight / total)
        column = lax.dynamic_index_in_dim(similar, class_picks[turn_index].astype(jnp.int32), 1, keepdims=False)
        cover = jnp.maximum(cover, column)
    return jnp.stack(scores), cover * weight


def score_item(packed):
    return class_scores(packed[0], packed[1], packed[2])


def reference(sketches, labels, places, counts, chosen):
    flat_index = (labels * BLOCK + places).astype(jnp.int32)
    blocks = jnp.zeros((CLASSES * BLOCK, D), sketches.dtype).at[flat_index].set(sketches)
    blocks = blocks.reshape(CLASSES, BLOCK, D)
    scores, cover = lax.map(score_item, (blocks, counts, jnp.transpose(chosen)))
    return jnp.transpose(scores, (1, 0, 2)), cover
```

```python
import jax
import jax.numpy as jnp
from jax import lax
from jax.experimental import pallas as pl
from jax.experimental.pallas import tpu as pltpu
from jax.sharding import PartitionSpec as P

MESH = pl.DeviceIdType.MESH
D = 4096
BIG = 1e30
PARTS = ((0, 1408), (1408, 1408), (2816, 1280))
UNIT = 32
BS = 512
NB = 8
EXT = 16
TASKS = 18


def my_coords():
    dp = lax.axis_index("dp")
    cls = lax.axis_index("cls")
    return dp // 2, (cls // 2) % 4, (dp % 2) * 2 + cls // 8, cls % 2


def device_at(x, y, z, core):
    return (x * 2 + z // 2, ((z % 2) * 4 + y) * 2 + core)


def class_at(y, z):
    return (z % 2) * 8 + y * 2 + z // 2


def plane(part, x, y, z, a, b):
    if part == 0:
        ty, tz = (y + a) % 4, (z + b) % 4
        return (x, ty, tz), class_at(ty, tz)
    if part == 1:
        tx, tz = (x + a) % 4, (z + b) % 4
        return (tx, y, tz), class_at((tx - tz + 4) % 4, tz)
    tx, ty = (x + a) % 4, (y + b) % 4
    return (tx, ty, z), class_at(ty, (tx - ty + 4) % 4)


def exchange_kernel(out_ref, vrow_ref, pick_ref, block_ref, vpart_ref, ppart_ref, relay0, relay1, relay2,
                    send1, recv1, send2, recv2, dsend, drecv, asend, arecv):
    x, y, z, core = my_coords()
    owner_x = (y + z) % 4
    owner_y = (x - z + 4) % 4
    owner_z = (x - y + 4) % 4
    is_owner = x == owner_x
    relays = (relay0, relay1, relay2)
    partner = device_at(x, y, z, 1 - core)

    aux = (
        pltpu.make_async_remote_copy(vrow_ref, vpart_ref, asend.at[0], arecv.at[0], device_id=partner, device_id_type=MESH),
        pltpu.make_async_remote_copy(pick_ref, ppart_ref, asend.at[1], arecv.at[1], device_id=partner, device_id_type=MESH),
    )
    for copy in aux:
        copy.start()

    order = [(a, b) for a in range(4) for b in range(4)]
    first = []
    for i, (a, b) in enumerate(order):
        for part, (start, size) in enumerate(PARTS):
            if (a, b) == (0, 0):
                continue
            (tx, ty, tz), klass = plane(part, x, y, z, a, b)
            copy = pltpu.make_async_remote_copy(
                out_ref.at[pl.ds(pl.multiple_of(klass * UNIT, UNIT), UNIT), pl.ds(start, size)],
                relays[part].at[i],
                send1.at[part, i],
                recv1.at[part, i],
                device_id=device_at(tx, ty, tz, core),
                device_id_type=MESH,
            )
            copy.start()
            first.append((part, i, copy))

    def forward(part, i, a, b, source):
        start, size = PARTS[part]
        if part == 0:
            sx, sy, sz = x, (y - a + 4) % 4, (z - b + 4) % 4
            target, d = (owner_x, y, z), (x - owner_x + 4) % 4
        elif part == 1:
            sx, sy, sz = (x - a + 4) % 4, y, (z - b + 4) % 4
            target, d = (x, owner_y, z), (y - owner_y + 4) % 4
        else:
            sx, sy, sz = (x - a + 4) % 4, (y - b + 4) % 4, z
            target, d = (x, y, owner_z), (z - owner_z + 4) % 4
        dest = block_ref.at[core, sx, sz, sy, :, pl.ds(start, size)]
        there = pltpu.make_async_remote_copy(
            source, dest, send2.at[part, i], recv2.at[part, d],
            device_id=device_at(*target, core), device_id_type=MESH,
        )
        here = pltpu.make_async_copy(source, dest, send2.at[part, i])
        return there, here

    second = []
    for i, (a, b) in enumerate(order):
        for part, (start, size) in enumerate(PARTS):
            if (a, b) == (0, 0):
                _, klass = plane(part, x, y, z, 0, 0)
                source = out_ref.at[pl.ds(pl.multiple_of(klass * UNIT, UNIT), UNIT), pl.ds(start, size)]
            else:
                source = relays[part].at[i]
                for p, n, copy in first:
                    if (p, n) == (part, i):
                        copy.wait_recv()
            there, here = forward(part, i, a, b, source)

            @pl.when(jnp.logical_not(is_owner))
            def _():
                there.start()

            @pl.when(is_owner)
            def _():
                here.start()

            second.append((there, here))

    def region(part, n, half):
        start, size = PARTS[part]
        if part == 0:
            return block_ref.at[half, n, :, :, :, pl.ds(start, size)]
        if part == 1:
            return block_ref.at[half, :, :, n, :, pl.ds(start, size)]
        return block_ref.at[half, :, n, :, :, pl.ds(start, size)]

    @pl.when(jnp.logical_not(is_owner))
    def _():
        for there, _ in second:
            there.wait_send()

    @pl.when(is_owner)
    def _():
        for _, here in second:
            here.wait()
        across = []
        for d in range(4):
            for part in range(3):
                n = ((x, y, z)[part] + d) % 4
                piece = region(part, n, core)
                if d:
                    pltpu.make_async_copy(piece, piece, recv2.at[part, d]).wait()
                copy = pltpu.make_async_remote_copy(
                    piece, piece, dsend.at[part, d], drecv.at[part, d], device_id=partner, device_id_type=MESH
                )
                copy.start()
                across.append(copy)
        for copy in across:
            copy.wait()

    for _, _, copy in first:
        copy.wait_send()
    for copy in aux:
        copy.wait()


def exchange(outgoing, vrow, pick):
    anywhere = pl.BlockSpec(memory_space=pl.ANY)
    vmem = pl.BlockSpec(memory_space=pltpu.VMEM)
    block, vpart, ppart = pl.pallas_call(
        exchange_kernel,
        out_shape=(
            jax.ShapeDtypeStruct((2, 4, 4, 4, UNIT, D), jnp.bfloat16),
            jax.ShapeDtypeStruct(vrow.shape, vrow.dtype),
            jax.ShapeDtypeStruct(pick.shape, pick.dtype),
        ),
        in_specs=[vmem, vmem, vmem],
        out_specs=(anywhere, vmem, vmem),
        scratch_shapes=[pltpu.VMEM((16, UNIT, size), jnp.bfloat16) for _, size in PARTS]
        + [
            pltpu.SemaphoreType.DMA((3, 16)),
            pltpu.SemaphoreType.DMA((3, 16)),
            pltpu.SemaphoreType.DMA((3, 16)),
            pltpu.SemaphoreType.DMA((3, 4)),
            pltpu.SemaphoreType.DMA((3, 4)),
            pltpu.SemaphoreType.DMA((3, 4)),
            pltpu.SemaphoreType.DMA((2,)),
            pltpu.SemaphoreType.DMA((2,)),
        ],
        compiler_params=pltpu.CompilerParams(has_side_effects=True),
        name="exchange",
    )(outgoing, vrow, pick)
    return block.reshape(NB, BS, D), vpart, ppart


def column(row):
    return jnp.broadcast_to(row, (128, row.shape[1])).T


def score_kernel(pick_ref, block_ref, valid_ref, res_ref, xs, gram, hcol, a1col, a2col, r1, r2, rg, rows, sums, peak,
                 pbuf, sems, psem):
    dp = lax.axis_index("dp")
    cls = lax.axis_index("cls")
    x, y, z = dp // 2, (cls // 2) % 4, (dp % 2) * 2 + cls // 8
    core = cls % 2
    res_ref[...] = jnp.zeros_like(res_ref)

    @pl.when(x == (y + z) % 4)
    def _():
        loads = [
            pltpu.make_async_copy(block_ref.at[b], xs.at[b, pl.ds(0, BS)], sems.at[b]) for b in range(NB)
        ]
        for t in range(3):
            c = pick_ref[0, t]
            pltpu.make_async_copy(
                block_ref.at[c // BS, pl.ds(pl.multiple_of(c % BS // 16 * 16, 16), 16)], pbuf.at[t], psem.at[t]
            ).start()
        for copy in loads:
            copy.start()
        picked = jnp.zeros((EXT, D), jnp.float32)
        line = lax.broadcasted_iota(jnp.int32, (EXT, D), 0)
        hp = []
        for t in range(3):
            c = pick_ref[0, t]
            pltpu.make_async_copy(pbuf.at[t], pbuf.at[t], psem.at[t]).wait()
            wide = pbuf[t].astype(jnp.float32)
            one = jnp.sum(jnp.where(line == c % 16, wide, 0.0), axis=0, keepdims=True)
            hp.append(0.5 * jnp.sum(one * one, axis=1, keepdims=True))
            picked = jnp.where(line == t, one, picked)
        picked = picked.astype(jnp.bfloat16)
        r1[...] = jnp.zeros_like(r1)
        r2[...] = jnp.zeros_like(r2)
        rg[...] = jnp.zeros_like(rg)
        sums[...] = jnp.zeros_like(sums)
        peak[...] = jnp.zeros_like(peak)

        def norms(b, carry):
            pltpu.make_async_copy(block_ref.at[b], xs.at[b, pl.ds(0, BS)], sems.at[b]).wait()
            xs[b, pl.ds(BS, EXT)] = picked

            def strip(i, c):
                wide = xs[b, pl.ds(pl.multiple_of(i * 32, 32), 32)].astype(jnp.float32)
                h = 0.5 * jnp.sum(wide * wide, axis=1, keepdims=True)
                hcol[b, pl.ds(pl.multiple_of(i * 32, 32), 32)] = jnp.broadcast_to(h, (32, 128))
                return c

            lax.fori_loop(0, BS // 32, strip, 0)
            hrow = hcol[b].T[0:1]
            good = valid_ref[b] > 0.0
            own = b // 4 == core
            res_ref[4, b] = jnp.where(own, hrow, 0.0)[0]
            rows[b, 0:1] = jnp.where(good[0:1], hrow, -BIG)
            hcol[b] = column(rows[b, 0:1])
            return carry

        lax.fori_loop(0, NB, norms, 0)

        def task(n, carry):
            is_diag = n < 4
            pair = n - 4
            inner_i = jnp.where(pair < 3, 0, jnp.where(pair < 5, 1, 2))
            inner_j = jnp.where(pair < 3, pair + 1, jnp.where(pair < 5, pair - 1, 3))
            cross = n - 10
            ci = jnp.where(core == 0, cross % 4, 6 + cross % 2)
            cj = jnp.where(core == 0, 4 + cross // 4, cross // 2)
            i = jnp.where(is_diag, 4 * core + n, jnp.where(n < 10, 4 * core + inner_i, ci))
            j = jnp.where(is_diag, 4 * core + n, jnp.where(n < 10, 4 * core + inner_j, cj))
            gram[...] = lax.dot_general(
                xs[i], xs[j, pl.ds(0, BS)], (((1,), (1,)), ((), ())), preferred_element_type=jnp.float32
            )
            near = gram[pl.ds(BS, 8)]
            good = valid_ref[j][0:1] > 0.0
            p1 = hp[0] - near[0:1]
            p2 = jnp.minimum(p1, hp[1] - near[1:2])
            p3 = jnp.minimum(p2, hp[2] - near[2:3])
            a1 = jnp.where(good, p1, -BIG)
            a2 = jnp.where(good, p2, -BIG)
            rows[j, 1:2] = a1
            rows[j, 2:3] = a2

            @pl.when(is_diag)
            def _():
                a1col[j] = column(a1)
                a2col[j] = column(a2)
                res_ref[3, j] = p3[0]

            hu_all = rows[j, 0:1]

            def strip(k, c):
                base = pl.multiple_of(k * 32, 32)
                hq = hcol[i, pl.ds(base, 32)]
                a1q = a1col[i, pl.ds(base, 32)]
                a2q = a2col[i, pl.ds(base, 32)]
                off = jnp.logical_not(is_diag)
                t1 = jnp.zeros((32, 128), jnp.float32)
                t2 = t1
                tg = t1
                top = peak[...]
                for cb in range(4):
                    lanes = pl.ds(cb * 128, 128)
                    g = gram[pl.ds(base, 32), lanes]
                    e = g - rows[j, 0:1, lanes]
                    f = g - hq
                    gap = hq - e
                    top = jnp.maximum(top, jnp.maximum(jnp.maximum(gap[0:8], gap[8:16]), jnp.maximum(gap[16:24], gap[24:32])))
                    u1 = jnp.maximum(e + a1q, 0.0)
                    u2 = jnp.maximum(e + a2q, 0.0)
                    sums[j, 0, :, lanes] += (u1[0:8] + u1[8:16]) + (u1[16:24] + u1[24:32])
                    sums[j, 1, :, lanes] += (u2[0:8] + u2[8:16]) + (u2[16:24] + u2[24:32])
                    sums[j, 2, :, lanes] += (g[0:8] + g[8:16]) + (g[16:24] + g[24:32])
                    t1 += jnp.maximum(f + rows[j, 1:2, lanes], 0.0)
                    t2 += jnp.maximum(f + rows[j, 2:3, lanes], 0.0)
                    tg += g
                peak[...] = top

                @pl.when(off)
                def _():
                    r1[i, pl.ds(base, 32)] += t1
                    r2[i, pl.ds(base, 32)] += t2
                    rg[i, pl.ds(base, 32)] += tg

                return c

            lax.fori_loop(0, BS // 32, strip, 0)
            return carry

        lax.fori_loop(0, TASKS, task, 0)

        def finish(b, carry):
            for n, part in enumerate((r1, r2, rg)):
                across = jnp.sum(part[b].T, axis=0, keepdims=True)
                res_ref[n, b] = (across + jnp.sum(sums[b, n], axis=0, keepdims=True))[0]
            return carry

        lax.fori_loop(0, NB, finish, 0)
        best = jnp.max(jnp.max(peak[...], axis=0, keepdims=True), axis=1, keepdims=True)
        for b in range(NB):
            res_ref[5, b] = jnp.broadcast_to(best, (1, BS))[0]


def scores(block, valid, pick):
    return pl.pallas_call(
        score_kernel,
        out_shape=jax.ShapeDtypeStruct((8, NB, BS), jnp.float32),
        in_specs=[
            pl.BlockSpec(memory_space=pltpu.SMEM),
            pl.BlockSpec(memory_space=pl.ANY),
            pl.BlockSpec(memory_space=pltpu.VMEM),
        ],
        out_specs=pl.BlockSpec(memory_space=pltpu.VMEM),
        scratch_shapes=[
            pltpu.VMEM((NB, BS + EXT, D), jnp.bfloat16),
            pltpu.VMEM((BS + EXT, BS), jnp.float32),
            pltpu.VMEM((NB, BS, 128), jnp.float32),
            pltpu.VMEM((NB, BS, 128), jnp.float32),
            pltpu.VMEM((NB, BS, 128), jnp.float32),
            pltpu.VMEM((NB, BS, 128), jnp.float32),
            pltpu.VMEM((NB, BS, 128), jnp.float32),
            pltpu.VMEM((NB, BS, 128), jnp.float32),
            pltpu.VMEM((NB, 8, BS), jnp.float32),
            pltpu.VMEM((NB, 3, 8, BS), jnp.float32),
            pltpu.VMEM((8, 128), jnp.float32),
            pltpu.VMEM((3, EXT, D), jnp.bfloat16),
            pltpu.SemaphoreType.DMA((NB,)),
            pltpu.SemaphoreType.DMA((3,)),
        ],
        compiler_params=pltpu.CompilerParams(vmem_limit_bytes=62 * 1024 * 1024),
        name="scores",
    )(pick, block, valid)


def spread_kernel(res_ref, all_ref, send, recv):
    x, y, z, core = my_coords()
    klass = class_at(y, z)
    me = lax.axis_index("dp")
    cls = lax.axis_index("cls")
    is_owner = x == (y + z) % 4

    @pl.when(is_owner)
    def _():
        copies = []
        for m in range(8):
            local = jnp.logical_and(me == m, cls == klass)
            there = pltpu.make_async_remote_copy(
                res_ref, all_ref.at[core], send.at[m], recv.at[core], device_id=(m, klass), device_id_type=MESH
            )

            @pl.when(jnp.logical_not(local))
            def _():
                there.start()

            @pl.when(local)
            def _():
                pltpu.make_async_copy(res_ref, all_ref.at[core], recv.at[core]).start()

            copies.append((local, there))
        for local, there in copies:

            @pl.when(jnp.logical_not(local))
            def _():
                there.wait_send()

    for c in range(2):
        pltpu.make_async_copy(all_ref.at[c], all_ref.at[c], recv.at[c]).wait()


def share(res):
    vmem = pl.BlockSpec(memory_space=pltpu.VMEM)
    anywhere = pl.BlockSpec(memory_space=pl.ANY)
    return pl.pallas_call(
        spread_kernel,
        out_shape=jax.ShapeDtypeStruct((2, 8, 4096), jnp.float32),
        in_specs=[vmem],
        out_specs=anywhere,
        scratch_shapes=[pltpu.SemaphoreType.DMA((8,)), pltpu.SemaphoreType.DMA((2,))],
        compiler_params=pltpu.CompilerParams(has_side_effects=True),
        name="share",
    )(res)


def body(sketches, labels, places, counts, chosen):
    member = lax.axis_index("dp")
    row_count = sketches.shape[0]
    target = labels * UNIT + places // 512 * 4 + places % 4
    table = (lax.broadcasted_iota(jnp.int32, (512, row_count), 0) == target[None, :]).astype(jnp.bfloat16)
    outgoing = jnp.dot(table, sketches, preferred_element_type=jnp.float32).astype(jnp.bfloat16)

    class_counts = counts[0]
    picked = chosen[:, 0]
    source = picked % 512 // 4
    where = source % 2 * 2048 + source // 2 * UNIT + picked // 512 * 4 + picked % 4
    pick = jnp.zeros((8, 128), jnp.int32).at[0, :3].set(where)
    by_source = class_counts.reshape(8, 64, 2)
    valid = jnp.arange(4, dtype=jnp.int32) < jnp.transpose(by_source, (2, 1, 0))[..., None]
    valid = valid.reshape(NB, 1, BS).astype(jnp.float32)

    block, vpart, ppart = exchange(outgoing, valid, pick)
    mine = lax.axis_index("cls") % 2 == member % 2
    valid_k = jnp.where(mine, valid, vpart)
    pick_k = jnp.where(mine, pick, ppart)
    res = scores(block, valid_k, pick_k)
    both = share(res.reshape(8, 4096))

    def mine_of(rows):
        cut = lax.dynamic_index_in_dim(rows.reshape(-1, 2, 64, 8, 4), member, 3, keepdims=False)
        return jnp.transpose(cut, (0, 2, 1, 3)).reshape(-1, 512)

    total = jnp.sum(class_counts).astype(jnp.float32)
    scale = 2.0 / D
    bound = jnp.maximum(both[0, 5, 0], both[1, 5, 0]) * scale
    joined = both[0, :5] + both[1, :5]
    all_h = jnp.sum(joined[4])
    cut = mine_of(joined)
    own_counts = lax.dynamic_index_in_dim(class_counts, member, 0, keepdims=False)
    own_valid = (jnp.arange(4, dtype=jnp.int32)[None, :] < own_counts[:, None]).reshape(512)
    far = total * cut[4] + all_h - cut[2]
    gains = jnp.stack([total * bound - far * scale, cut[0] * scale, cut[1] * scale])
    gain_scores = jnp.where(own_valid[None, :], gains, 0.0) / total
    coverage = jnp.where(own_valid, jnp.maximum(bound - (cut[4] + cut[3]) * scale, 0.0), 0.0)
    return (gain_scores[:, None, :], coverage[None, :])


def solution(mesh):
    placed = (
        P(("dp", "cls"), None),
        P(("dp", "cls")),
        P(("dp", "cls")),
        P("cls", None, None),
        P(None, "cls"),
    )
    return jax.shard_map(
        body,
        mesh=mesh,
        in_specs=placed,
        out_specs=(P(None, "cls", "dp"), P("cls", "dp")),
        check_vma=False,
    )
```

```python
import jax
import jax.numpy as jnp
from jax import lax
from jax.experimental import pallas as pl
from jax.experimental.pallas import tpu as pltpu
from jax.sharding import PartitionSpec as P

MESH = pl.DeviceIdType.MESH
D = 4096
BIG = 1e30
SCALE = 2.0 / D
PARTS = ((0, 1408), (1408, 1408), (2816, 1280))
UNIT = 32
STEPS = 16
BS = 512
HALF = 2048
EXT = 16
SKEW_Y = 1
SKEW_Z = 3


def my_coords():
    dp = lax.axis_index("dp")
    cls = lax.axis_index("cls")
    return dp // 2, (cls // 2) % 4, (dp % 2) * 2 + cls // 8, cls % 2


def device_at(x, y, z, core):
    return (x * 2 + z // 2, ((z % 2) * 4 + y) * 2 + core)


def class_at(y, z):
    return (z % 2) * 8 + y * 2 + z // 2


def both_true(a, b, c):
    return jnp.logical_and(jnp.logical_and(a, b), c)


def repeat(count, step):
    def once(n, carry):
        step(n)
        return carry

    lax.fori_loop(0, count, once, 0)


def column(row):
    return jnp.broadcast_to(row, (128, row.shape[1])).T


def fold(v):
    return (v[0:8] + v[8:16]) + (v[16:24] + v[24:32])


def kernel(pick_ref, out_ref, valid_ref, all_ref, xs, relay0, relay1, relay2, gram, tab, hcol, a1col, a2col,
           r1, r2, rg, sums, peak, part, got, final, pacc, send1, recv1, send2, rstep, dsend, drecv, tsend, trecv, msend, mrecv):
    x, y, z, core = my_coords()
    relays = (relay0, relay1, relay2)
    is_owner = x == (y + z) % 4
    partner = device_at(x, y, z, 1 - core)
    klass = class_at(y, z)

    def place_of(half, n, sx, start, size):
        return xs.at[half, n // 4, pl.ds(pl.multiple_of(n % 4 * 128 + sx * UNIT, UNIT), UNIT), pl.ds(start, size)]

    def sends(n, wait):
        oy = (y - SKEW_Y * x - n // 4 + 16) % 4
        oz = (z - SKEW_Z * x - n % 4 + 16) % 4
        ox = (oy + oz) % 4
        to = class_at(oy, oz)
        for p, (start, size) in enumerate(PARTS):
            rx, ry, rz = ((x, oy, oz), (ox, y, oz), (ox, oy, z))[p]
            own = both_true(rx == x, ry == y, rz == z)
            last = both_true(rx == ox, ry == oy, rz == oz)
            source = out_ref.at[pl.ds(pl.multiple_of(to * UNIT, UNIT), UNIT), pl.ds(start, size)]
            dest = place_of(core, n, x, start, size)
            via = pltpu.make_async_remote_copy(
                source, relays[p].at[n], send1.at[p, n], recv1.at[p, n],
                device_id=device_at(rx, ry, rz, core), device_id_type=MESH,
            )
            direct = pltpu.make_async_remote_copy(
                source, dest, send1.at[p, n], rstep.at[n],
                device_id=device_at(ox, oy, oz, core), device_id_type=MESH,
            )
            here = jnp.logical_and(own, last)
            if wait:

                @pl.when(jnp.logical_not(here))
                def _():
                    direct.wait_send()

            else:

                @pl.when(jnp.logical_not(jnp.logical_or(own, last)))
                def _():
                    via.start()

                @pl.when(jnp.logical_xor(own, last))
                def _():
                    direct.start()

                @pl.when(here)
                def _():
                    pltpu.make_async_copy(source, dest, rstep.at[n]).start()

    def forwards(n, wait):
        for p, (start, size) in enumerate(PARTS):
            if p == 0:
                oy, oz = y, z
                sx = x
            elif p == 1:
                oy, oz = (x - z + 4) % 4, z
                sx = (SKEW_Y * (y - oy - n // 4) + 16) % 4
            else:
                oy, oz = y, (x - y + 4) % 4
                sx = (SKEW_Z * (z - oz - n % 4 + 8)) % 4
            ox = (oy + oz) % 4
            sy = (oy + SKEW_Y * sx + n // 4) % 4
            sz = (oz + SKEW_Z * sx + n % 4) % 4
            mine = both_true(sx == x, sy == y, sz == z)
            copy = pltpu.make_async_remote_copy(
                relays[p].at[n], place_of(core, n, sx, start, size), send2.at[p, n], rstep.at[n],
                device_id=device_at(ox, oy, oz, core), device_id_type=MESH,
            )

            @pl.when(jnp.logical_not(mine))
            def _():
                if wait:
                    copy.wait_send()
                else:
                    pltpu.make_async_copy(relays[p].at[n], relays[p].at[n], recv1.at[p, n]).wait()
                    copy.start()

    repeat(STEPS, lambda n: sends(n, False))

    @pl.when(jnp.logical_not(is_owner))
    def _():
        repeat(STEPS, lambda n: forwards(n, False))
        repeat(STEPS, lambda n: forwards(n, True))

    def tile(half, s, r, slot):
        gram[slot] = lax.dot_general(
            xs[half, s], xs[core, r], (((1,), (1,)), ((), ())), preferred_element_type=jnp.float32
        )

    def across(r):
        return pltpu.make_async_remote_copy(
            xs.at[core, r], xs.at[core, r], dsend.at[r], drecv.at[r], device_id=partner, device_id_type=MESH
        )

    def share_copy(m):
        return pltpu.make_async_remote_copy(
            final, all_ref.at[core], msend.at[m], mrecv.at[core], device_id=(m, klass), device_id_type=MESH
        )

    @pl.when(is_owner)
    def _():
        other = 1 - core
        pacc[...] = jnp.zeros_like(pacc)

        def take(half, r):
            pacc[...] += jnp.dot(pick_ref[half, r], xs[half, r], preferred_element_type=jnp.float32)

        def round_of(r):
            for q in range(4):
                rows = xs.at[core, r, pl.ds(q * 128, 128)]
                pltpu.make_async_copy(rows, rows, rstep.at[r * 4 + q]).wait()
            across(r).start()

            take(core, r)

            def own_tile(s, carry):
                tile(core, s, r, r * (r + 1) // 2 + s)
                return carry

            lax.fori_loop(0, r + 1, own_tile, 0)

            @pl.when(r > 0)
            def _():
                across(r - 1).wait_recv()
                take(other, r - 1)

                @pl.when((r - 1) % 2 == core)
                def _():
                    tile(other, r - 1, r - 1, 16 + (r - 1) // 2)

            def cross_tile(s, carry):
                tile(other, s, r, 10 + r * (r - 1) // 2 + s)
                return carry

            lax.fori_loop(0, r, cross_tile, 0)

        repeat(4, round_of)
        across(3).wait_recv()
        take(other, 3)

        @pl.when(core == 1)
        def _():
            tile(other, 3, 3, 17)

        wide = pacc[...]
        hp = [0.5 * jnp.sum(wide[t : t + 1] * wide[t : t + 1], axis=1, keepdims=True) for t in range(3)]
        picked = wide.astype(jnp.bfloat16)

        eye = lax.broadcasted_iota(jnp.int32, (128, 128), 0) == lax.broadcasted_iota(jnp.int32, (128, 128), 1)

        def group(n, xx):
            ny = (y + SKEW_Y * xx + n // 4) % 4
            nz = (z + SKEW_Z * xx + n % 4) % 4
            return ny, nz

        lane = lax.broadcasted_iota(jnp.int32, (8, 128), 1) // UNIT

        def own_rows(r):
            near = lax.dot_general(
                picked, xs[core, r], (((1,), (1,)), ((), ())), preferred_element_type=jnp.float32
            )
            for q in range(4):
                n = r * 4 + q
                lanes = slice(q * 128, q * 128 + 128)
                sub = gram[r * (r + 3) // 2, lanes, lanes]
                h = 0.5 * jnp.sum(jnp.where(eye, sub, 0.0), axis=0, keepdims=True)
                good = jnp.zeros((8, 128), jnp.float32)
                for xx in range(4):
                    ny, nz = group(n, xx)
                    piece = jnp.broadcast_to(valid_ref[core * 16 + xx * 4 + ny], (8, 128))
                    good = jnp.where(lane == xx, pltpu.roll(piece, (xx - nz + 4) % 4 * UNIT, 1), good)
                ok = good[0:1] > 0.0
                p1 = hp[0] - near[0:1, lanes]
                p2 = jnp.minimum(p1, hp[1] - near[1:2, lanes])
                p3 = jnp.minimum(p2, hp[2] - near[2:3, lanes])
                tab[core, r, 0:1, lanes] = jnp.where(ok, h, -BIG)
                tab[core, r, 1:2, lanes] = jnp.where(ok, p1, -BIG)
                tab[core, r, 2:3, lanes] = jnp.where(ok, p2, -BIG)
                tab[core, r, 3:4, lanes] = p3
                tab[core, r, 4:5, lanes] = h
                tab[core, r, 5:6, lanes] = good[0:1]

        repeat(4, own_rows)
        sums[...] = jnp.zeros_like(sums)
        peak[...] = jnp.zeros_like(peak)
        tables = pltpu.make_async_remote_copy(
            tab.at[core], tab.at[core], tsend.at[0], trecv.at[0], device_id=partner, device_id_type=MESH
        )

        def row_block(b):
            half = jnp.where(b < 4, core, other)
            s = b % 4
            mine = b < 4

            @pl.when(b == 1)
            def _():
                tables.start()

            @pl.when(b == 4)
            def _():
                tables.wait()

            hcol[...] = column(tab[half, s, 0:1])
            a1col[...] = column(tab[half, s, 1:2])
            a2col[...] = column(tab[half, s, 2:3])
            r1[...] = jnp.zeros_like(r1)
            r2[...] = jnp.zeros_like(r2)
            rg[...] = jnp.zeros_like(rg)

            def one_tile(r, carry):
                slot = jnp.where(
                    mine, r * (r + 1) // 2 + s, jnp.where(r == s, 16 + s // 2, 10 + r * (r - 1) // 2 + s)
                )
                diag = jnp.logical_and(mine, r == s)

                def sweep(rows_too):
                    for cb in range(4):
                        lanes = slice(cb * 128, cb * 128 + 128)
                        hu = tab[core, r, 0:1, lanes]
                        a1u = tab[core, r, 1:2, lanes]
                        a2u = tab[core, r, 2:3, lanes]

                        def strip(k, acc):
                            c1, c2, cg, top = acc
                            at = pl.ds(pl.multiple_of(k * 32, 32), 32)
                            g = gram[slot, at, lanes]
                            hq = hcol[at]
                            e = g - hu
                            gap = hq - e
                            c1 = c1 + fold(jnp.maximum(e + a1col[at], 0.0))
                            c2 = c2 + fold(jnp.maximum(e + a2col[at], 0.0))
                            cg = cg + fold(g)
                            top = jnp.maximum(
                                top, jnp.maximum(jnp.maximum(gap[0:8], gap[8:16]), jnp.maximum(gap[16:24], gap[24:32]))
                            )
                            if rows_too:
                                f = g - hq
                                r1[at] += jnp.maximum(f + a1u, 0.0)
                                r2[at] += jnp.maximum(f + a2u, 0.0)
                                rg[at] += g
                            return c1, c2, cg, top

                        zero = jnp.zeros((8, 128), jnp.float32)
                        c1, c2, cg, top = lax.fori_loop(0, BS // 32, strip, (zero, zero, zero, peak[...]), unroll=4)
                        sums[r, 0, :, lanes] += c1
                        sums[r, 1, :, lanes] += c2
                        sums[r, 2, :, lanes] += cg
                        peak[...] = top

                @pl.when(diag)
                def _():
                    sweep(False)

                @pl.when(jnp.logical_not(diag))
                def _():
                    sweep(True)

                return carry

            begin = jnp.where(jnp.logical_or(mine, s % 2 == core), s, s + 1)
            lax.fori_loop(begin, 4, one_tile, 0)
            for n, acc in enumerate((r1, r2, rg)):
                part[half, s, n : n + 1] = jnp.sum(acc[...].T, axis=0, keepdims=True)

        repeat(8, row_block)
        best = jnp.max(jnp.max(peak[...], axis=0, keepdims=True), axis=1, keepdims=True)
        for r in range(4):
            part[other, r, 3:4] = jnp.broadcast_to(best, (1, BS))
        partial = pltpu.make_async_remote_copy(
            part.at[other], got, tsend.at[1], trecv.at[1], device_id=partner, device_id_type=MESH
        )
        total = jnp.sum(jnp.sum(valid_ref[...], axis=0), axis=1, keepdims=True)
        h_sum = jnp.zeros((1, 1), jnp.float32)
        for half in range(2):
            for r in range(4):
                h_sum = h_sum + jnp.sum(tab[half, r, 4:5], axis=1, keepdims=True)
        partial.start()
        partial.wait()
        bound = jnp.maximum(best, got[0, 3:4, 0:1]) * SCALE

        for r in range(4):
            cols = [jnp.sum(sums[r, n], axis=0, keepdims=True) + part[core, r, n : n + 1] + got[r, n : n + 1] for n in range(3)]
            h = tab[core, r, 4:5]
            ok = tab[core, r, 5:6] > 0.0
            far = total * h + h_sum - cols[2]
            part[core, r, 4:5] = jnp.where(ok, (total * bound - far * SCALE) / total, 0.0)
            part[core, r, 5:6] = jnp.where(ok, cols[0] * SCALE / total, 0.0)
            part[core, r, 6:7] = jnp.where(ok, cols[1] * SCALE / total, 0.0)
            part[core, r, 7:8] = jnp.where(ok, jnp.maximum(bound - (h + tab[core, r, 3:4]) * SCALE, 0.0), 0.0)

        def natural(n):
            xx, ny = n // 4, n % 4
            i1 = (ny - y - SKEW_Y * xx + 16) % 4
            piece = jnp.zeros((8, 128), jnp.float32)
            for nz in range(4):
                i2 = (nz - z - SKEW_Z * xx + 16) % 4
                take = part[core, i1, :, pl.ds(pl.multiple_of(i2 * 128, 128), 128)]
                piece = jnp.where(lane == nz, pltpu.roll(take, (nz - xx + 4) % 4 * UNIT, 1), piece)
            final[:, pl.ds(pl.multiple_of(n * 128, 128), 128)] = piece[4:8]

        repeat(16, natural)
        me = lax.axis_index("dp")
        cls = lax.axis_index("cls")
        for m in range(8):
            local = jnp.logical_and(me == m, cls == klass)

            @pl.when(jnp.logical_not(local))
            def _():
                share_copy(m).start()

            @pl.when(local)
            def _():
                all_ref[core] = final[...]

        for m in range(8):
            local = jnp.logical_and(me == m, cls == klass)

            @pl.when(jnp.logical_not(local))
            def _():
                share_copy(m).wait_send()

        repeat(4, lambda r: across(r).wait_send())

    repeat(STEPS, lambda n: sends(n, True))
    cls = lax.axis_index("cls")
    for c in range(2):
        local = both_true(is_owner, core == c, cls == klass)

        @pl.when(jnp.logical_not(local))
        def _():
            pltpu.make_async_copy(all_ref.at[c], all_ref.at[c], mrecv.at[c]).wait()


def select_facilities(outgoing, valid, pick):
    vmem = pl.BlockSpec(memory_space=pltpu.VMEM)
    sems = pltpu.SemaphoreType.DMA
    wide = pltpu.VMEM((BS, 128), jnp.float32)
    return pl.pallas_call(
        kernel,
        out_shape=jax.ShapeDtypeStruct((2, 4, HALF), jnp.float32),
        in_specs=[vmem, pl.BlockSpec(memory_space=pl.ANY), vmem],
        out_specs=vmem,
        scratch_shapes=[pltpu.VMEM((2, 4, BS, D), jnp.bfloat16)]
        + [pltpu.VMEM((STEPS, UNIT, size), jnp.bfloat16) for _, size in PARTS]
        + [
            pltpu.VMEM((18, BS, BS), jnp.float32),
            pltpu.VMEM((2, 4, 8, BS), jnp.float32),
            wide, wide, wide, wide, wide, wide,
            pltpu.VMEM((4, 3, 8, BS), jnp.float32),
            pltpu.VMEM((8, 128), jnp.float32),
            pltpu.VMEM((2, 4, 8, BS), jnp.float32),
            pltpu.VMEM((4, 8, BS), jnp.float32),
            pltpu.VMEM((4, HALF), jnp.float32),
            pltpu.VMEM((EXT, D), jnp.float32),
            sems((3, STEPS)), sems((3, STEPS)), sems((3, STEPS)), sems((STEPS,)),
            sems((4,)), sems((4,)), sems((2,)), sems((2,)), sems((8,)), sems((2,)),
        ],
        compiler_params=pltpu.CompilerParams(has_side_effects=True, vmem_limit_bytes=62 * 1024 * 1024),
        name="facilities",
    )(pick, outgoing, valid)


def body(sketches, labels, places, counts, chosen):
    member = lax.axis_index("dp")
    cls = lax.axis_index("cls")
    row_count = sketches.shape[0]
    info = jnp.concatenate([counts[0], jnp.pad(chosen[:, :1], ((0, 5), (0, 127)))], axis=0)
    swapped = lax.ppermute(info, "cls", [(n, n ^ 1) for n in range(16)])
    target = labels * UNIT + places // 512 * 4 + places % 4
    table = (lax.broadcasted_iota(jnp.int32, (512, row_count), 0) == target[None, :]).astype(jnp.bfloat16)
    outgoing = jnp.dot(table, sketches, preferred_element_type=jnp.float32).astype(jnp.bfloat16)

    x, y, z, core = member // 2, (cls // 2) % 4, (member % 2) * 2 + cls // 8, cls % 2
    info = jnp.where(core == z // 2, info, swapped)
    picked = info[8:11, 0]
    source = picked % 512 // 4
    sx, sz, sy, score = source // 32, source // 8 % 4, source // 2 % 4, source % 2
    step = (sy - y - SKEW_Y * sx + 16) % 4 * 4 + (sz - z - SKEW_Z * sx + 16) % 4
    where = score * HALF + step * 128 + sx * UNIT + picked // 512 * 4 + picked % 4
    spot = jnp.pad(where, (0, EXT - 3), constant_values=-1)
    line = jnp.arange(4096, dtype=jnp.int32).reshape(8, 1, BS)
    pick = (line == spot[None, :, None]).astype(jnp.bfloat16).reshape(2, 4, EXT, BS)
    by_source = jnp.transpose(info[:8].reshape(8, 4, 4, 4, 2), (4, 1, 3, 2, 0))
    valid = (jnp.arange(4, dtype=jnp.int32) < by_source[..., None]).astype(jnp.float32).reshape(32, 1, 128)

    both = select_facilities(outgoing, valid, pick)
    cut = lax.dynamic_index_in_dim(both.reshape(2, 4, 4, 4, 4, 8, 4), member, 5, keepdims=False)
    rows = jnp.transpose(cut, (1, 2, 4, 3, 0, 5)).reshape(4, 512)
    return (rows[:3, None, :], rows[3:4])


def solution(mesh):
    placed = (
        P(("dp", "cls"), None),
        P(("dp", "cls")),
        P(("dp", "cls")),
        P("cls", None, None),
        P(None, "cls"),
    )
    return jax.shard_map(
        body,
        mesh=mesh,
        in_specs=placed,
        out_specs=(P(None, "cls", "dp"), P("cls", "dp")),
        check_vma=False,
    )
```

```python
import jax
import jax.numpy as jnp
from jax import lax
from jax.experimental import pallas as pl
from jax.experimental.pallas import tpu as pltpu
from jax.sharding import PartitionSpec as P

MESH = pl.DeviceIdType.MESH
D = 4096
BIG = 1e30
SCALE = 2.0 / D
PARTS = ((0, 1408), (1408, 1408), (2816, 1280))
UNIT = 32
STEPS = 16
BS = 512
HALF = 2048
EXT = 16
SKEW_Y = 1
SKEW_Z = 3


def my_coords():
    dp = lax.axis_index("dp")
    cls = lax.axis_index("cls")
    return dp // 2, (cls // 2) % 4, (dp % 2) * 2 + cls // 8, cls % 2


def device_at(x, y, z, core):
    return (x * 2 + z // 2, ((z % 2) * 4 + y) * 2 + core)


def class_at(y, z):
    return (z % 2) * 8 + y * 2 + z // 2


def both_true(a, b, c):
    return jnp.logical_and(jnp.logical_and(a, b), c)


def repeat(count, step):
    def once(n, carry):
        step(n)
        return carry

    lax.fori_loop(0, count, once, 0)


def column(row):
    return jnp.broadcast_to(row, (128, row.shape[1])).T


def fold(v):
    return (v[0:8] + v[8:16]) + (v[16:24] + v[24:32])


def kernel(pick_ref, out_ref, valid_ref, gain_ref, cover_ref, xs, relay0, relay1, relay2, gram, tab, hcol, a1col, a2col,
           r1, r2, rg, sums, peak, part, got, final, pacc, landed, send1, recv1, send2, rstep, dsend, drecv, tsend, trecv, msend, mrecv):
    x, y, z, core = my_coords()
    relays = (relay0, relay1, relay2)
    is_owner = x == (y + z) % 4
    partner = device_at(x, y, z, 1 - core)
    klass = class_at(y, z)

    def place_of(half, n, sx, start, size):
        return xs.at[half, n // 4, pl.ds(pl.multiple_of(n % 4 * 128 + sx * UNIT, UNIT), UNIT), pl.ds(start, size)]

    def beside(p, owner):
        line = (owner[p] + 1 + 2 * (owner[p] % 2)) % 4
        return line, tuple(line if q == p else owner[q] for q in range(3))

    def detour(p, n, owner, source, sem):
        _, chip = beside(p, owner)
        slot = STEPS + n // 2
        copy = pltpu.make_async_remote_copy(
            source, relays[p].at[slot], sem, recv1.at[p, slot],
            device_id=device_at(*chip, core), device_id_type=MESH,
        )
        return jnp.logical_and(((x, y, z)[p] - owner[p] + 4) % 4 == 2, n % 2 == 1), copy

    def sends(n, wait):
        oy = (y - SKEW_Y * x - n // 4 + 16) % 4
        oz = (z - SKEW_Z * x - n % 4 + 16) % 4
        ox = (oy + oz) % 4
        to = class_at(oy, oz)
        for p, (start, size) in enumerate(PARTS):
            rx, ry, rz = ((x, oy, oz), (ox, y, oz), (ox, oy, z))[p]
            own = both_true(rx == x, ry == y, rz == z)
            last = both_true(rx == ox, ry == oy, rz == oz)
            source = out_ref.at[pl.ds(pl.multiple_of(to * UNIT, UNIT), UNIT), pl.ds(start, size)]
            dest = place_of(core, n, x, start, size)
            via = pltpu.make_async_remote_copy(
                source, relays[p].at[n], send1.at[p, n], recv1.at[p, n],
                device_id=device_at(rx, ry, rz, core), device_id_type=MESH,
            )
            direct = pltpu.make_async_remote_copy(
                source, dest, send1.at[p, n], rstep.at[n],
                device_id=device_at(ox, oy, oz, core), device_id_type=MESH,
            )
            here = jnp.logical_and(own, last)
            aside, bypass = detour(p, n, (ox, oy, oz), source, send1.at[p, n])
            aside = jnp.logical_and(own, aside)
            if wait:

                @pl.when(jnp.logical_not(here))
                def _():
                    direct.wait_send()

            else:

                @pl.when(jnp.logical_not(jnp.logical_or(own, last)))
                def _():
                    via.start()

                @pl.when(jnp.logical_and(jnp.logical_xor(own, last), jnp.logical_not(aside)))
                def _():
                    direct.start()

                @pl.when(aside)
                def _():
                    bypass.start()

                @pl.when(here)
                def _():
                    pltpu.make_async_copy(source, dest, rstep.at[n]).start()

    def line_owner(p):
        if p == 0:
            return (y + z) % 4, y, z
        if p == 1:
            return x, (x - z + 4) % 4, z
        return x, y, (x - y + 4) % 4

    def source_of(p, n, owner, line):
        _, oy, oz = owner
        if p == 0:
            sx = line
        elif p == 1:
            sx = (SKEW_Y * (line - oy - n // 4) + 16) % 4
        else:
            sx = (SKEW_Z * (line - oz - n % 4 + 8)) % 4
        return sx, (oy + SKEW_Y * sx + n // 4) % 4, (oz + SKEW_Z * sx + n % 4) % 4

    def pass_on(p, n, slot, owner, sx):
        start, size = PARTS[p]
        return pltpu.make_async_remote_copy(
            relays[p].at[slot], place_of(core, n, sx, start, size), send2.at[p, slot], rstep.at[n],
            device_id=device_at(*owner, core), device_id_type=MESH,
        )

    def arrived(p, slot):
        pltpu.make_async_copy(relays[p].at[slot], relays[p].at[slot], recv1.at[p, slot]).wait()

    def forwards(n, wait):
        for p in range(3):
            owner = line_owner(p)
            here = (x, y, z)[p]
            sx, sy, sz = source_of(p, n, owner, here)
            mine = both_true(sx == x, sy == y, sz == z)
            copy = pass_on(p, n, n, owner, sx)
            aside, bypass = detour(p, n, owner, relays[p].at[n], send2.at[p, n])

            @pl.when(jnp.logical_not(mine))
            def _():
                if wait:
                    copy.wait_send()
                else:
                    arrived(p, n)

                    @pl.when(aside)
                    def _():
                        bypass.start()

                    @pl.when(jnp.logical_not(aside))
                    def _():
                        copy.start()

            slot = STEPS + n // 2
            fx, _, _ = source_of(p, n, owner, (owner[p] + 2) % 4)
            far = pass_on(p, n, slot, owner, fx)

            @pl.when(jnp.logical_and(here == beside(p, owner)[0], n % 2 == 1))
            def _():
                if wait:
                    far.wait_send()
                else:
                    arrived(p, slot)
                    far.start()

    repeat(STEPS, lambda n: sends(n, False))

    @pl.when(jnp.logical_not(is_owner))
    def _():
        repeat(STEPS, lambda n: forwards(n, False))
        repeat(STEPS, lambda n: forwards(n, True))

    def tile(half, s, r, slot):
        gram[slot] = lax.dot_general(
            xs[half, s], xs[core, r], (((1,), (1,)), ((), ())), preferred_element_type=jnp.float32
        )

    def half_tile(half, s, h, slot):
        lines = pl.ds(pl.multiple_of(h * 256, 256), 256)
        gram[slot, :, lines] = lax.dot_general(
            xs[half, s], xs[core, 3, lines], (((1,), (1,)), ((), ())), preferred_element_type=jnp.float32
        )

    def across(r):
        return pltpu.make_async_remote_copy(
            xs.at[core, r], xs.at[core, r], dsend.at[r], drecv.at[r], device_id=partner, device_id_type=MESH
        )

    def across_half(h):
        rows = xs.at[core, 3, pl.ds(pl.multiple_of(h * 256, 256), 256)]
        return pltpu.make_async_remote_copy(
            rows, rows, dsend.at[3 + h], drecv.at[3 + h], device_id=partner, device_id_type=MESH
        )

    def share_copy(m):
        return pltpu.make_async_remote_copy(
            final.at[m], landed.at[core], msend.at[m], mrecv.at[core], device_id=(m, klass), device_id_type=MESH
        )

    @pl.when(is_owner)
    def _():
        other = 1 - core
        pacc[...] = jnp.zeros_like(pacc)

        def take(half, r):
            pacc[...] += jnp.dot(pick_ref[half, r], xs[half, r], preferred_element_type=jnp.float32)

        def steps_in(r, first, count):
            for q in range(count):
                rows = xs.at[core, r, pl.ds(pl.multiple_of((first + q) * 128, 128), 128)]
                pltpu.make_async_copy(rows, rows, rstep.at[r * 4 + first + q]).wait()

        def other_in(r):
            across(r).wait_recv()
            take(other, r)

            @pl.when(r % 2 == core)
            def _():
                tile(other, r, r, 16 + r // 2)

        def round_of(r):
            steps_in(r, 0, 4)
            across(r).start()
            take(core, r)

            def own_tile(s, carry):
                tile(core, s, r, r * (r + 1) // 2 + s)
                return carry

            lax.fori_loop(0, r + 1, own_tile, 0)

            @pl.when(r > 0)
            def _():
                other_in(r - 1)

            def cross_tile(s, carry):
                tile(other, s, r, 10 + r * (r - 1) // 2 + s)
                return carry

            lax.fori_loop(0, r, cross_tile, 0)

        repeat(3, round_of)

        def last_half(h):
            steps_in(3, 2 * h, 2)
            across_half(h).start()
            repeat(3, lambda s: half_tile(core, s, h, 6 + s))

            @pl.when(h == 0)
            def _():
                other_in(2)

            repeat(3, lambda s: half_tile(other, s, h, 13 + s))

        repeat(2, last_half)
        take(core, 3)
        tile(core, 3, 3, 9)
        for h in range(2):
            across_half(h).wait_recv()
        take(other, 3)

        @pl.when(core == 1)
        def _():
            tile(other, 3, 3, 17)

        wide = pacc[...]
        hp = [0.5 * jnp.sum(wide[t : t + 1] * wide[t : t + 1], axis=1, keepdims=True) for t in range(3)]
        picked = wide.astype(jnp.bfloat16)

        eye = lax.broadcasted_iota(jnp.int32, (128, 128), 0) == lax.broadcasted_iota(jnp.int32, (128, 128), 1)

        def group(n, xx):
            ny = (y + SKEW_Y * xx + n // 4) % 4
            nz = (z + SKEW_Z * xx + n % 4) % 4
            return ny, nz

        lane = lax.broadcasted_iota(jnp.int32, (8, 128), 1) // UNIT

        def own_rows(r):
            near = lax.dot_general(
                picked, xs[core, r], (((1,), (1,)), ((), ())), preferred_element_type=jnp.float32
            )
            for q in range(4):
                n = r * 4 + q
                lanes = slice(q * 128, q * 128 + 128)
                sub = gram[r * (r + 3) // 2, lanes, lanes]
                h = 0.5 * jnp.sum(jnp.where(eye, sub, 0.0), axis=0, keepdims=True)
                good = jnp.zeros((8, 128), jnp.float32)
                for xx in range(4):
                    ny, nz = group(n, xx)
                    piece = jnp.broadcast_to(valid_ref[core * 16 + xx * 4 + ny], (8, 128))
                    good = jnp.where(lane == xx, pltpu.roll(piece, (xx - nz + 4) % 4 * UNIT, 1), good)
                ok = good[0:1] > 0.0
                p1 = hp[0] - near[0:1, lanes]
                p2 = jnp.minimum(p1, hp[1] - near[1:2, lanes])
                p3 = jnp.minimum(p2, hp[2] - near[2:3, lanes])
                tab[core, r, 0:1, lanes] = jnp.where(ok, h, -BIG)
                tab[core, r, 1:2, lanes] = jnp.where(ok, p1, -BIG)
                tab[core, r, 2:3, lanes] = jnp.where(ok, p2, -BIG)
                tab[core, r, 3:4, lanes] = p3
                tab[core, r, 4:5, lanes] = h
                tab[core, r, 5:6, lanes] = good[0:1]

        repeat(4, own_rows)
        sums[...] = jnp.zeros_like(sums)
        peak[...] = jnp.zeros_like(peak)
        tables = pltpu.make_async_remote_copy(
            tab.at[core], tab.at[core], tsend.at[0], trecv.at[0], device_id=partner, device_id_type=MESH
        )

        def row_block(b):
            half = jnp.where(b < 4, core, other)
            s = b % 4
            mine = b < 4

            @pl.when(b == 1)
            def _():
                tables.start()

            @pl.when(b == 4)
            def _():
                tables.wait()

            hcol[...] = column(tab[half, s, 0:1])
            a1col[...] = column(tab[half, s, 1:2])
            a2col[...] = column(tab[half, s, 2:3])
            r1[...] = jnp.zeros_like(r1)
            r2[...] = jnp.zeros_like(r2)
            rg[...] = jnp.zeros_like(rg)

            def one_tile(r, carry):
                slot = jnp.where(
                    mine, r * (r + 1) // 2 + s, jnp.where(r == s, 16 + s // 2, 10 + r * (r - 1) // 2 + s)
                )
                diag = jnp.logical_and(mine, r == s)

                def sweep(rows_too):
                    for cb in range(4):
                        lanes = slice(cb * 128, cb * 128 + 128)
                        hu = tab[core, r, 0:1, lanes]
                        a1u = tab[core, r, 1:2, lanes]
                        a2u = tab[core, r, 2:3, lanes]

                        def strip(k, acc):
                            c1, c2, cg, top = acc
                            at = pl.ds(pl.multiple_of(k * 32, 32), 32)
                            g = gram[slot, at, lanes]
                            hq = hcol[at]
                            e = g - hu
                            gap = hq - e
                            c1 = c1 + fold(jnp.maximum(e + a1col[at], 0.0))
                            c2 = c2 + fold(jnp.maximum(e + a2col[at], 0.0))
                            cg = cg + fold(g)
                            top = jnp.maximum(
                                top, jnp.maximum(jnp.maximum(gap[0:8], gap[8:16]), jnp.maximum(gap[16:24], gap[24:32]))
                            )
                            if rows_too:
                                f = g - hq
                                r1[at] += jnp.maximum(f + a1u, 0.0)
                                r2[at] += jnp.maximum(f + a2u, 0.0)
                                rg[at] += g
                            return c1, c2, cg, top

                        zero = jnp.zeros((8, 128), jnp.float32)
                        c1, c2, cg, top = lax.fori_loop(0, BS // 32, strip, (zero, zero, zero, peak[...]), unroll=4)
                        sums[r, 0, :, lanes] += c1
                        sums[r, 1, :, lanes] += c2
                        sums[r, 2, :, lanes] += cg
                        peak[...] = top

                @pl.when(diag)
                def _():
                    sweep(False)

                @pl.when(jnp.logical_not(diag))
                def _():
                    sweep(True)

                return carry

            begin = jnp.where(jnp.logical_or(mine, s % 2 == core), s, s + 1)
            lax.fori_loop(begin, 4, one_tile, 0)
            for n, acc in enumerate((r1, r2, rg)):
                part[half, s, n : n + 1] = jnp.sum(acc[...].T, axis=0, keepdims=True)

        repeat(8, row_block)
        best = jnp.max(jnp.max(peak[...], axis=0, keepdims=True), axis=1, keepdims=True)
        for r in range(4):
            part[other, r, 3:4] = jnp.broadcast_to(best, (1, BS))
        partial = pltpu.make_async_remote_copy(
            part.at[other], got, tsend.at[1], trecv.at[1], device_id=partner, device_id_type=MESH
        )
        total = jnp.sum(jnp.sum(valid_ref[...], axis=0), axis=1, keepdims=True)
        h_sum = jnp.zeros((1, 1), jnp.float32)
        for half in range(2):
            for r in range(4):
                h_sum = h_sum + jnp.sum(tab[half, r, 4:5], axis=1, keepdims=True)
        partial.start()
        partial.wait()
        bound = jnp.maximum(best, got[0, 3:4, 0:1]) * SCALE

        for r in range(4):
            cols = [jnp.sum(sums[r, n], axis=0, keepdims=True) + part[core, r, n : n + 1] + got[r, n : n + 1] for n in range(3)]
            h = tab[core, r, 4:5]
            ok = tab[core, r, 5:6] > 0.0
            far = total * h + h_sum - cols[2]
            part[core, r, 4:5] = jnp.where(ok, (total * bound - far * SCALE) / total, 0.0)
            part[core, r, 5:6] = jnp.where(ok, cols[0] * SCALE / total, 0.0)
            part[core, r, 6:7] = jnp.where(ok, cols[1] * SCALE / total, 0.0)
            part[core, r, 7:8] = jnp.where(ok, jnp.maximum(bound - (h + tab[core, r, 3:4]) * SCALE, 0.0), 0.0)

        def natural(n):
            xx, ny = n // 4, n % 4
            i1 = (ny - y - SKEW_Y * xx + 16) % 4
            piece = jnp.zeros((8, 128), jnp.float32)
            for nz in range(4):
                i2 = (nz - z - SKEW_Z * xx + 16) % 4
                take = part[core, i1, :, pl.ds(pl.multiple_of(i2 * 128, 128), 128)]
                piece = jnp.where(lane == nz, pltpu.roll(take, (nz - xx + 4) % 4 * UNIT, 1), piece)
            seat = lax.broadcasted_iota(jnp.int32, (8, 128), 1) % UNIT // 4 == 2 * ny + core
            for m in range(8):
                spot = pltpu.roll(piece, (2 * ny + core - m + 32) * 4 % 128, 1)
                final[m, :, pl.ds(pl.multiple_of(xx * 128, 128), 128)] += jnp.where(seat, spot, 0.0)[4:8]

        final[...] = jnp.zeros_like(final)
        repeat(16, natural)
        me = lax.axis_index("dp")
        cls = lax.axis_index("cls")
        for m in range(8):
            local = jnp.logical_and(me == m, cls == klass)

            @pl.when(jnp.logical_not(local))
            def _():
                share_copy(m).start()

            @pl.when(local)
            def _():
                landed[core] = final[m]

        for m in range(8):
            local = jnp.logical_and(me == m, cls == klass)

            @pl.when(jnp.logical_not(local))
            def _():
                share_copy(m).wait_send()

        repeat(3, lambda r: across(r).wait_send())
        repeat(2, lambda h: across_half(h).wait_send())

    repeat(STEPS, lambda n: sends(n, True))
    cls = lax.axis_index("cls")
    for c in range(2):
        local = both_true(is_owner, core == c, cls == klass)

        @pl.when(jnp.logical_not(local))
        def _():
            pltpu.make_async_copy(landed.at[c], landed.at[c], mrecv.at[c]).wait()

    rows = landed[0] + landed[1]
    for t in range(3):
        gain_ref[t] = rows[t : t + 1]
    cover_ref[...] = rows[3:4]


def select_facilities(outgoing, valid, pick):
    vmem = pl.BlockSpec(memory_space=pltpu.VMEM)
    sems = pltpu.SemaphoreType.DMA
    wide = pltpu.VMEM((BS, 128), jnp.float32)
    return pl.pallas_call(
        kernel,
        out_shape=(jax.ShapeDtypeStruct((3, 1, BS), jnp.float32), jax.ShapeDtypeStruct((1, BS), jnp.float32)),
        in_specs=[vmem, pl.BlockSpec(memory_space=pl.ANY), vmem],
        out_specs=(vmem, vmem),
        scratch_shapes=[pltpu.VMEM((2, 4, BS, D), jnp.bfloat16)]
        + [pltpu.VMEM((STEPS + STEPS // 2, UNIT, size), jnp.bfloat16) for _, size in PARTS]
        + [
            pltpu.VMEM((18, BS, BS), jnp.float32),
            pltpu.VMEM((2, 4, 8, BS), jnp.float32),
            wide, wide, wide, wide, wide, wide,
            pltpu.VMEM((4, 3, 8, BS), jnp.float32),
            pltpu.VMEM((8, 128), jnp.float32),
            pltpu.VMEM((2, 4, 8, BS), jnp.float32),
            pltpu.VMEM((4, 8, BS), jnp.float32),
            pltpu.VMEM((8, 4, BS), jnp.float32),
            pltpu.VMEM((EXT, D), jnp.float32),
            pltpu.VMEM((2, 4, BS), jnp.float32),
            sems((3, STEPS)), sems((3, STEPS + STEPS // 2)), sems((3, STEPS + STEPS // 2)), sems((STEPS,)),
            sems((5,)), sems((5,)), sems((2,)), sems((2,)), sems((8,)), sems((2,)),
        ],
        compiler_params=pltpu.CompilerParams(has_side_effects=True, vmem_limit_bytes=62 * 1024 * 1024),
        name="facilities",
    )(pick, outgoing, valid)


def body(sketches, labels, places, counts, chosen):
    member = lax.axis_index("dp")
    cls = lax.axis_index("cls")
    row_count = sketches.shape[0]
    info = jnp.concatenate([counts[0], jnp.pad(chosen[:, :1], ((0, 5), (0, 127)))], axis=0)
    swapped = lax.ppermute(info, "cls", [(n, n ^ 1) for n in range(16)])
    target = labels * UNIT + places // 512 * 4 + places % 4
    table = (lax.broadcasted_iota(jnp.int32, (512, row_count), 0) == target[None, :]).astype(jnp.bfloat16)
    outgoing = jnp.dot(table, sketches, preferred_element_type=jnp.float32).astype(jnp.bfloat16)

    x, y, z, core = member // 2, (cls // 2) % 4, (member % 2) * 2 + cls // 8, cls % 2
    info = jnp.where(core == z // 2, info, swapped)
    picked = info[8:11, 0]
    source = picked % 512 // 4
    sx, sz, sy, score = source // 32, source // 8 % 4, source // 2 % 4, source % 2
    step = (sy - y - SKEW_Y * sx + 16) % 4 * 4 + (sz - z - SKEW_Z * sx + 16) % 4
    where = score * HALF + step * 128 + sx * UNIT + picked // 512 * 4 + picked % 4
    spot = jnp.pad(where, (0, EXT - 3), constant_values=-1)
    line = jnp.arange(4096, dtype=jnp.int32).reshape(8, 1, BS)
    pick = (line == spot[None, :, None]).astype(jnp.bfloat16).reshape(2, 4, EXT, BS)
    by_source = jnp.transpose(info[:8].reshape(8, 4, 4, 4, 2), (4, 1, 3, 2, 0))
    valid = (jnp.arange(4, dtype=jnp.int32) < by_source[..., None]).astype(jnp.float32).reshape(32, 1, 128)

    return select_facilities(outgoing, valid, pick)


def solution(mesh):
    placed = (
        P(("dp", "cls"), None),
        P(("dp", "cls")),
        P(("dp", "cls")),
        P("cls", None, None),
        P(None, "cls"),
    )
    return jax.shard_map(
        body,
        mesh=mesh,
        in_specs=placed,
        out_specs=(P(None, "cls", "dp"), P("cls", "dp")),
        check_vma=False,
    )
```

```python
import jax
import jax.numpy as jnp
from jax import lax
from jax.experimental import pallas as pl
from jax.experimental.pallas import tpu as pltpu
from jax.sharding import PartitionSpec as P

MESH = pl.DeviceIdType.MESH
D = 4096
BIG = 1e30
SCALE = 2.0 / D
PARTS = ((0, 1408), (1408, 1408), (2816, 1280))
UNIT = 32
STEPS = 16
BS = 512
HALF = 2048
EXT = 16
SKEW_Y = 1
SKEW_Z = 3


def my_coords():
    dp = lax.axis_index("dp")
    cls = lax.axis_index("cls")
    return dp // 2, (cls // 2) % 4, (dp % 2) * 2 + cls // 8, cls % 2


def device_at(x, y, z, core):
    return (x * 2 + z // 2, ((z % 2) * 4 + y) * 2 + core)


def class_at(y, z):
    return (z % 2) * 8 + y * 2 + z // 2


def both_true(a, b, c):
    return jnp.logical_and(jnp.logical_and(a, b), c)


def repeat(count, step):
    def once(n, carry):
        step(n)
        return carry

    lax.fori_loop(0, count, once, 0)


def column(row):
    return jnp.broadcast_to(row, (128, row.shape[1])).T


def fold(v):
    return (v[0:8] + v[8:16]) + (v[16:24] + v[24:32])


def kernel(pick_ref, out_ref, valid_ref, landed, xs, relay0, relay1, relay2, gram, tab, hcol, a1col, a2col,
           r1, r2, sums, peak, part, got, final, pacc, send1, recv1, send2, rstep, dsend, drecv, tsend, trecv, msend, mrecv):
    x, y, z, core = my_coords()
    relays = (relay0, relay1, relay2)
    is_owner = x == (y + z) % 4
    partner = device_at(x, y, z, 1 - core)
    klass = class_at(y, z)

    def place_of(half, n, sx, start, size):
        return xs.at[half, n // 4, pl.ds(pl.multiple_of(n % 4 * 128 + sx * UNIT, UNIT), UNIT), pl.ds(start, size)]

    def beside(p, owner):
        line = (owner[p] + 1 + 2 * (owner[p] % 2)) % 4
        return line, tuple(line if q == p else owner[q] for q in range(3))

    def detour(p, n, owner, source, sem):
        _, chip = beside(p, owner)
        slot = STEPS + n // 2
        copy = pltpu.make_async_remote_copy(
            source, relays[p].at[slot], sem, recv1.at[p, slot],
            device_id=device_at(*chip, core), device_id_type=MESH,
        )
        return jnp.logical_and(((x, y, z)[p] - owner[p] + 4) % 4 == 2, n % 2 == 1), copy

    def sends(n, wait):
        oy = (y - SKEW_Y * x - n // 4 + 16) % 4
        oz = (z - SKEW_Z * x - n % 4 + 16) % 4
        ox = (oy + oz) % 4
        to = class_at(oy, oz)
        for p, (start, size) in enumerate(PARTS):
            rx, ry, rz = ((x, oy, oz), (ox, y, oz), (ox, oy, z))[p]
            own = both_true(rx == x, ry == y, rz == z)
            last = both_true(rx == ox, ry == oy, rz == oz)
            source = out_ref.at[pl.ds(pl.multiple_of(to * UNIT, UNIT), UNIT), pl.ds(start, size)]
            dest = place_of(core, n, x, start, size)
            via = pltpu.make_async_remote_copy(
                source, relays[p].at[n], send1.at[p, n], recv1.at[p, n],
                device_id=device_at(rx, ry, rz, core), device_id_type=MESH,
            )
            direct = pltpu.make_async_remote_copy(
                source, dest, send1.at[p, n], rstep.at[n],
                device_id=device_at(ox, oy, oz, core), device_id_type=MESH,
            )
            here = jnp.logical_and(own, last)
            aside, bypass = detour(p, n, (ox, oy, oz), source, send1.at[p, n])
            aside = jnp.logical_and(own, aside)
            if wait:

                @pl.when(jnp.logical_not(here))
                def _():
                    direct.wait_send()

            else:

                @pl.when(jnp.logical_not(jnp.logical_or(own, last)))
                def _():
                    via.start()

                @pl.when(jnp.logical_and(jnp.logical_xor(own, last), jnp.logical_not(aside)))
                def _():
                    direct.start()

                @pl.when(aside)
                def _():
                    bypass.start()

                @pl.when(here)
                def _():
                    pltpu.make_async_copy(source, dest, rstep.at[n]).start()

    def line_owner(p):
        if p == 0:
            return (y + z) % 4, y, z
        if p == 1:
            return x, (x - z + 4) % 4, z
        return x, y, (x - y + 4) % 4

    def source_of(p, n, owner, line):
        _, oy, oz = owner
        if p == 0:
            sx = line
        elif p == 1:
            sx = (SKEW_Y * (line - oy - n // 4) + 16) % 4
        else:
            sx = (SKEW_Z * (line - oz - n % 4 + 8)) % 4
        return sx, (oy + SKEW_Y * sx + n // 4) % 4, (oz + SKEW_Z * sx + n % 4) % 4

    def pass_on(p, n, slot, owner, sx):
        start, size = PARTS[p]
        return pltpu.make_async_remote_copy(
            relays[p].at[slot], place_of(core, n, sx, start, size), send2.at[p, slot], rstep.at[n],
            device_id=device_at(*owner, core), device_id_type=MESH,
        )

    def arrived(p, slot):
        pltpu.make_async_copy(relays[p].at[slot], relays[p].at[slot], recv1.at[p, slot]).wait()

    def forwards(n, wait):
        for p in range(3):
            owner = line_owner(p)
            here = (x, y, z)[p]
            sx, sy, sz = source_of(p, n, owner, here)
            mine = both_true(sx == x, sy == y, sz == z)
            copy = pass_on(p, n, n, owner, sx)
            aside, bypass = detour(p, n, owner, relays[p].at[n], send2.at[p, n])

            @pl.when(jnp.logical_not(mine))
            def _():
                if wait:
                    copy.wait_send()
                else:
                    arrived(p, n)

                    @pl.when(aside)
                    def _():
                        bypass.start()

                    @pl.when(jnp.logical_not(aside))
                    def _():
                        copy.start()

            slot = STEPS + n // 2
            fx, _, _ = source_of(p, n, owner, (owner[p] + 2) % 4)
            far = pass_on(p, n, slot, owner, fx)

            @pl.when(jnp.logical_and(here == beside(p, owner)[0], n % 2 == 1))
            def _():
                if wait:
                    far.wait_send()
                else:
                    arrived(p, slot)
                    far.start()

    repeat(STEPS, lambda n: sends(n, False))

    @pl.when(jnp.logical_not(is_owner))
    def _():
        repeat(STEPS, lambda n: forwards(n, False))
        repeat(STEPS, lambda n: forwards(n, True))

    def tile(half, s, r, slot):
        gram[slot] = lax.dot_general(
            xs[half, s], xs[core, r], (((1,), (1,)), ((), ())), preferred_element_type=jnp.float32
        )

    def half_tile(half, s, h, slot):
        lines = pl.ds(pl.multiple_of(h * 256, 256), 256)
        gram[slot, :, lines] = lax.dot_general(
            xs[half, s], xs[core, 3, lines], (((1,), (1,)), ((), ())), preferred_element_type=jnp.float32
        )

    def across(r):
        return pltpu.make_async_remote_copy(
            xs.at[core, r], xs.at[core, r], dsend.at[r], drecv.at[r], device_id=partner, device_id_type=MESH
        )

    def across_half(h):
        rows = xs.at[core, 3, pl.ds(pl.multiple_of(h * 256, 256), 256)]
        return pltpu.make_async_remote_copy(
            rows, rows, dsend.at[3 + h], drecv.at[3 + h], device_id=partner, device_id_type=MESH
        )

    def share_copy(m):
        return pltpu.make_async_remote_copy(
            final.at[m], landed.at[core], msend.at[m], mrecv.at[core], device_id=(m, klass), device_id_type=MESH
        )

    @pl.when(is_owner)
    def _():
        other = 1 - core
        pacc[...] = jnp.zeros_like(pacc)

        def take(half, r):
            pacc[...] += jnp.dot(pick_ref[half, r], xs[half, r], preferred_element_type=jnp.float32)

        def steps_in(r, first, count):
            for q in range(count):
                rows = xs.at[core, r, pl.ds(pl.multiple_of((first + q) * 128, 128), 128)]
                pltpu.make_async_copy(rows, rows, rstep.at[r * 4 + first + q]).wait()

        def other_in(r):
            across(r).wait_recv()
            take(other, r)

            @pl.when(r % 2 == core)
            def _():
                tile(other, r, r, 16 + r // 2)

        def round_of(r):
            steps_in(r, 0, 4)
            across(r).start()
            take(core, r)

            def own_tile(s, carry):
                tile(core, s, r, r * (r + 1) // 2 + s)
                return carry

            lax.fori_loop(0, r + 1, own_tile, 0)

            @pl.when(r > 0)
            def _():
                other_in(r - 1)

            def cross_tile(s, carry):
                tile(other, s, r, 10 + r * (r - 1) // 2 + s)
                return carry

            lax.fori_loop(0, r, cross_tile, 0)

        repeat(3, round_of)

        def last_half(h):
            steps_in(3, 2 * h, 2)
            across_half(h).start()
            repeat(3, lambda s: half_tile(core, s, h, 6 + s))

            @pl.when(h == 0)
            def _():
                other_in(2)

            repeat(3, lambda s: half_tile(other, s, h, 13 + s))

        repeat(2, last_half)
        take(core, 3)
        tile(core, 3, 3, 9)
        for h in range(2):
            across_half(h).wait_recv()
        take(other, 3)

        @pl.when(core == 1)
        def _():
            tile(other, 3, 3, 17)

        wide = pacc[...]
        mass = wide[3:4]
        high = mass.astype(jnp.bfloat16).astype(jnp.float32)
        middle = (mass - high).astype(jnp.bfloat16).astype(jnp.float32)
        line = lax.broadcasted_iota(jnp.int32, (EXT, D), 0)
        hp = [0.5 * jnp.sum(wide[t : t + 1] * wide[t : t + 1], axis=1, keepdims=True) for t in range(3)]
        wide = jnp.where(line == 3, high, jnp.where(line == 4, middle, jnp.where(line == 5, mass - high - middle, wide)))
        picked = wide.astype(jnp.bfloat16)

        eye = lax.broadcasted_iota(jnp.int32, (128, 128), 0) == lax.broadcasted_iota(jnp.int32, (128, 128), 1)

        def group(n, xx):
            ny = (y + SKEW_Y * xx + n // 4) % 4
            nz = (z + SKEW_Z * xx + n % 4) % 4
            return ny, nz

        lane = lax.broadcasted_iota(jnp.int32, (8, 128), 1) // UNIT

        def own_rows(r):
            near = lax.dot_general(
                picked, xs[core, r], (((1,), (1,)), ((), ())), preferred_element_type=jnp.float32
            )
            for q in range(4):
                n = r * 4 + q
                lanes = slice(q * 128, q * 128 + 128)
                sub = gram[r * (r + 3) // 2, lanes, lanes]
                h = 0.5 * jnp.sum(jnp.where(eye, sub, 0.0), axis=0, keepdims=True)
                good = jnp.zeros((8, 128), jnp.float32)
                for xx in range(4):
                    ny, nz = group(n, xx)
                    piece = jnp.broadcast_to(valid_ref[core * 16 + xx * 4 + ny], (8, 128))
                    good = jnp.where(lane == xx, pltpu.roll(piece, (xx - nz + 4) % 4 * UNIT, 1), good)
                ok = good[0:1] > 0.0
                p1 = hp[0] - near[0:1, lanes]
                p2 = jnp.minimum(p1, hp[1] - near[1:2, lanes])
                p3 = jnp.minimum(p2, hp[2] - near[2:3, lanes])
                tab[core, r, 0:1, lanes] = jnp.where(ok, h, -BIG)
                tab[core, r, 1:2, lanes] = jnp.where(ok, p1, -BIG)
                tab[core, r, 2:3, lanes] = jnp.where(ok, p2, -BIG)
                tab[core, r, 3:4, lanes] = p3
                tab[core, r, 4:5, lanes] = h
                tab[core, r, 5:6, lanes] = good[0:1]
                tab[core, r, 6:7, lanes] = near[3:4, lanes] + near[4:5, lanes] + near[5:6, lanes]

        repeat(4, own_rows)
        sums[...] = jnp.zeros_like(sums)
        peak[...] = jnp.zeros_like(peak)
        tables = pltpu.make_async_remote_copy(
            tab.at[core], tab.at[core], tsend.at[0], trecv.at[0], device_id=partner, device_id_type=MESH
        )

        def row_block(b):
            half = jnp.where(b < 4, core, other)
            s = b % 4
            mine = b < 4

            @pl.when(b == 1)
            def _():
                tables.start()

            @pl.when(b == 4)
            def _():
                tables.wait()

            hcol[...] = column(tab[half, s, 0:1])
            a1col[...] = column(tab[half, s, 1:2])
            a2col[...] = column(tab[half, s, 2:3])
            r1[...] = jnp.zeros_like(r1)
            r2[...] = jnp.zeros_like(r2)

            def one_tile(r, carry):
                slot = jnp.where(
                    mine, r * (r + 1) // 2 + s, jnp.where(r == s, 16 + s // 2, 10 + r * (r - 1) // 2 + s)
                )
                diag = jnp.logical_and(mine, r == s)

                def sweep(rows_too):
                    for cb in range(4):
                        lanes = slice(cb * 128, cb * 128 + 128)
                        hu = tab[core, r, 0:1, lanes]
                        a1u = tab[core, r, 1:2, lanes]
                        a2u = tab[core, r, 2:3, lanes]

                        def strip(k, acc):
                            c1, c2, low = acc
                            at = pl.ds(pl.multiple_of(k * 32, 32), 32)
                            g = gram[slot, at, lanes]
                            e = g - hu
                            f = g - hcol[at]
                            c1 = c1 + fold(jnp.maximum(e + a1col[at], 0.0))
                            c2 = c2 + fold(jnp.maximum(e + a2col[at], 0.0))
                            low = jnp.minimum(
                                low, jnp.minimum(jnp.minimum(f[0:8], f[8:16]), jnp.minimum(f[16:24], f[24:32]))
                            )
                            if rows_too:
                                r1[at] += jnp.maximum(f + a1u, 0.0)
                                r2[at] += jnp.maximum(f + a2u, 0.0)
                            return c1, c2, low

                        zero = jnp.zeros((8, 128), jnp.float32)
                        c1, c2, low = lax.fori_loop(0, BS // 32, strip, (zero, zero, zero + BIG), unroll=4)
                        sums[r, 0, :, lanes] += c1
                        sums[r, 1, :, lanes] += c2
                        peak[...] = jnp.maximum(peak[...], hu - low)

                @pl.when(diag)
                def _():
                    sweep(False)

                @pl.when(jnp.logical_not(diag))
                def _():
                    sweep(True)

                return carry

            begin = jnp.where(jnp.logical_or(mine, s % 2 == core), s, s + 1)
            lax.fori_loop(begin, 4, one_tile, 0)
            for n, acc in enumerate((r1, r2)):
                part[half, s, n : n + 1] = jnp.sum(acc[...].T, axis=0, keepdims=True)

        repeat(8, row_block)
        best = jnp.max(jnp.max(peak[...], axis=0, keepdims=True), axis=1, keepdims=True)
        for r in range(4):
            part[other, r, 3:4] = jnp.broadcast_to(best, (1, BS))
        partial = pltpu.make_async_remote_copy(
            part.at[other], got, tsend.at[1], trecv.at[1], device_id=partner, device_id_type=MESH
        )
        total = jnp.sum(jnp.sum(valid_ref[...], axis=0), axis=1, keepdims=True)
        h_sum = jnp.zeros((1, 1), jnp.float32)
        for half in range(2):
            for r in range(4):
                h_sum = h_sum + jnp.sum(tab[half, r, 4:5], axis=1, keepdims=True)
        partial.start()
        partial.wait()
        bound = jnp.maximum(best, got[0, 3:4, 0:1]) * SCALE

        for r in range(4):
            cols = [jnp.sum(sums[r, n], axis=0, keepdims=True) + part[core, r, n : n + 1] + got[r, n : n + 1] for n in range(2)]
            h = tab[core, r, 4:5]
            ok = tab[core, r, 5:6] > 0.0
            far = total * h + h_sum - tab[core, r, 6:7]
            part[core, r, 4:5] = jnp.where(ok, (total * bound - far * SCALE) / total, 0.0)
            part[core, r, 5:6] = jnp.where(ok, cols[0] * SCALE / total, 0.0)
            part[core, r, 6:7] = jnp.where(ok, cols[1] * SCALE / total, 0.0)
            part[core, r, 7:8] = jnp.where(ok, jnp.maximum(bound - (h + tab[core, r, 3:4]) * SCALE, 0.0), 0.0)

        def natural(n):
            xx, ny = n // 4, n % 4
            i1 = (ny - y - SKEW_Y * xx + 16) % 4
            piece = jnp.zeros((8, 128), jnp.float32)
            for nz in range(4):
                i2 = (nz - z - SKEW_Z * xx + 16) % 4
                take = part[core, i1, :, pl.ds(pl.multiple_of(i2 * 128, 128), 128)]
                piece = jnp.where(lane == nz, pltpu.roll(take, (nz - xx + 4) % 4 * UNIT, 1), piece)
            seat = lax.broadcasted_iota(jnp.int32, (8, 128), 1) % UNIT // 4 == 2 * ny + core
            for m in range(8):
                spot = pltpu.roll(piece, (2 * ny + core - m + 32) * 4 % 128, 1)
                final[m, :, pl.ds(pl.multiple_of(xx * 128, 128), 128)] += jnp.where(seat, spot, 0.0)[4:8]

        final[...] = jnp.zeros_like(final)
        lax.fori_loop(0, 16, lambda n, carry: (natural(n), carry)[1], 0, unroll=4)
        me = lax.axis_index("dp")
        cls = lax.axis_index("cls")
        for m in range(8):
            local = jnp.logical_and(me == m, cls == klass)

            @pl.when(jnp.logical_not(local))
            def _():
                share_copy(m).start()

            @pl.when(local)
            def _():
                landed[core] = final[m]

        for m in range(8):
            local = jnp.logical_and(me == m, cls == klass)

            @pl.when(jnp.logical_not(local))
            def _():
                share_copy(m).wait_send()

        repeat(3, lambda r: across(r).wait_send())
        repeat(2, lambda h: across_half(h).wait_send())

    repeat(STEPS, lambda n: sends(n, True))
    cls = lax.axis_index("cls")
    for c in range(2):
        local = both_true(is_owner, core == c, cls == klass)

        @pl.when(jnp.logical_not(local))
        def _():
            pltpu.make_async_copy(landed.at[c], landed.at[c], mrecv.at[c]).wait()


def select_facilities(outgoing, valid, pick):
    vmem = pl.BlockSpec(memory_space=pltpu.VMEM)
    sems = pltpu.SemaphoreType.DMA
    wide = pltpu.VMEM((BS, 128), jnp.float32)
    return pl.pallas_call(
        kernel,
        out_shape=jax.ShapeDtypeStruct((2, 4, BS), jnp.float32),
        in_specs=[vmem, pl.BlockSpec(memory_space=pl.ANY), vmem],
        out_specs=vmem,
        scratch_shapes=[pltpu.VMEM((2, 4, BS, D), jnp.bfloat16)]
        + [pltpu.VMEM((STEPS + STEPS // 2, UNIT, size), jnp.bfloat16) for _, size in PARTS]
        + [
            pltpu.VMEM((18, BS, BS), jnp.float32),
            pltpu.VMEM((2, 4, 8, BS), jnp.float32),
            wide, wide, wide, wide, wide,
            pltpu.VMEM((4, 2, 8, BS), jnp.float32),
            pltpu.VMEM((8, 128), jnp.float32),
            pltpu.VMEM((2, 4, 8, BS), jnp.float32),
            pltpu.VMEM((4, 8, BS), jnp.float32),
            pltpu.VMEM((8, 4, BS), jnp.float32),
            pltpu.VMEM((EXT, D), jnp.float32),
            sems((3, STEPS)), sems((3, STEPS + STEPS // 2)), sems((3, STEPS + STEPS // 2)), sems((STEPS,)),
            sems((5,)), sems((5,)), sems((2,)), sems((2,)), sems((8,)), sems((2,)),
        ],
        compiler_params=pltpu.CompilerParams(has_side_effects=True, vmem_limit_bytes=62 * 1024 * 1024),
        name="facilities",
    )(pick, outgoing, valid)


def body(sketches, labels, places, counts, chosen):
    member = lax.axis_index("dp")
    cls = lax.axis_index("cls")
    row_count = sketches.shape[0]
    info = jnp.concatenate([counts[0], jnp.pad(chosen[:, :1], ((0, 5), (0, 127)))], axis=0)
    swapped = lax.ppermute(info, "cls", [(n, n ^ 1) for n in range(16)])
    target = labels * UNIT + places // 512 * 4 + places % 4
    table = (lax.broadcasted_iota(jnp.int32, (512, row_count), 0) == target[None, :]).astype(jnp.bfloat16)
    outgoing = jnp.dot(table, sketches, preferred_element_type=jnp.float32).astype(jnp.bfloat16)

    x, y, z, core = member // 2, (cls // 2) % 4, (member % 2) * 2 + cls // 8, cls % 2
    info = jnp.where(core == z // 2, info, swapped)
    picked = info[8:11, 0]
    source = picked % 512 // 4
    sx, sz, sy, score = source // 32, source // 8 % 4, source // 2 % 4, source % 2
    step = (sy - y - SKEW_Y * sx + 16) % 4 * 4 + (sz - z - SKEW_Z * sx + 16) % 4
    where = score * HALF + step * 128 + sx * UNIT + picked // 512 * 4 + picked % 4
    spot = jnp.pad(where, (0, EXT - 3), constant_values=-1)
    line = jnp.arange(4096, dtype=jnp.int32).reshape(8, 1, BS)
    everyone = jnp.arange(EXT, dtype=jnp.int32)[None, :, None] == 3
    pick = ((line == spot[None, :, None]) | everyone).astype(jnp.bfloat16).reshape(2, 4, EXT, BS)
    by_source = jnp.transpose(info[:8].reshape(8, 4, 4, 4, 2), (4, 1, 3, 2, 0))
    valid = (jnp.arange(4, dtype=jnp.int32) < by_source[..., None]).astype(jnp.float32).reshape(32, 1, 128)

    both = select_facilities(outgoing, valid, pick)
    return (both[0, :3, None, :] + both[1, :3, None, :], both[0, 3:] + both[1, 3:])


def solution(mesh):
    placed = (
        P(("dp", "cls"), None),
        P(("dp", "cls")),
        P(("dp", "cls")),
        P("cls", None, None),
        P(None, "cls"),
    )
    return jax.shard_map(
        body,
        mesh=mesh,
        in_specs=placed,
        out_specs=(P(None, "cls", "dp"), P("cls", "dp")),
        check_vma=False,
    )
```

```python
import jax
import jax.numpy as jnp
from jax import lax
from jax.experimental import pallas as pl
from jax.experimental.pallas import tpu as pltpu
from jax.sharding import PartitionSpec as P

MESH = pl.DeviceIdType.MESH
D = 4096
BIG = 1e30
SCALE = 2.0 / D
PARTS = ((0, 1408), (1408, 1408), (2816, 1280))
UNIT = 32
STEPS = 16
BS = 512
HALF = 2048
EXT = 16
SKEW_Y = 1
SKEW_Z = 3


def my_coords():
    dp = lax.axis_index("dp")
    cls = lax.axis_index("cls")
    return dp // 2, (cls // 2) % 4, (dp % 2) * 2 + cls // 8, cls % 2


def device_at(x, y, z, core):
    return (x * 2 + z // 2, ((z % 2) * 4 + y) * 2 + core)


def class_at(y, z):
    return (z % 2) * 8 + y * 2 + z // 2


def both_true(a, b, c):
    return jnp.logical_and(jnp.logical_and(a, b), c)


def repeat(count, step):
    def once(n, carry):
        step(n)
        return carry

    lax.fori_loop(0, count, once, 0)


def column(row):
    return jnp.broadcast_to(row, (128, row.shape[1])).T


def fold(v):
    return (v[0:8] + v[8:16]) + (v[16:24] + v[24:32])


def kernel(target_ref, sketch_ref, pick_ref, valid_ref, landed, xs, relay0, relay1, relay2, gram, tab, hcol, a1col, a2col,
           r1, r2, sums, peak, part, got, final, pacc, send1, recv1, send2, rstep, dsend, drecv, tsend, trecv, msend, mrecv, load_sem, credit):
    x, y, z, core = my_coords()
    relays = (relay0, relay1, relay2)
    is_owner = x == (y + z) % 4
    partner = device_at(x, y, z, 1 - core)
    klass = class_at(y, z)
    cls = lax.axis_index("cls")
    other = 1 - core
    out_ref = xs.at[other, 0]
    load = pltpu.make_async_copy(sketch_ref, xs.at[other, 1, pl.ds(0, 256)], load_sem)
    load.start()

    barrier = pltpu.get_barrier_semaphore()

    def greet(who):
        pl.semaphore_signal(barrier, inc=1, device_id=who, device_id_type=MESH)

    peers = [(a, b, c) for a in range(4) for b in range(4) for c in range(4) if 0 in (a, b, c) and (a, b, c) != (0, 0, 0)]
    for a, b, c in peers:
        greet(device_at((x + a) % 4, (y + b) % 4, (z + c) % 4, core))
    greet(partner)
    home_z = 2 * (cls % 2) + cls // 8
    home_x = (y + home_z) % 4
    for c in range(2):

        @pl.when(jnp.logical_not(both_true(home_x == x, home_z == z, core == c)))
        def _():
            greet(device_at(home_x, y, home_z, c))

    load.wait()
    table = (lax.broadcasted_iota(jnp.int32, (512, 256), 0) == target_ref[...]).astype(jnp.bfloat16)

    def place_slots(n):
        lanes = pl.ds(pl.multiple_of(n * 512, 512), 512)
        xs[other, 0, :, lanes] = jnp.dot(
            table, xs[other, 1, 0:256, lanes], preferred_element_type=jnp.float32
        ).astype(jnp.bfloat16)

    repeat(8, place_slots)
    members = jnp.where(cls == klass, 7, 8)
    pl.semaphore_wait(barrier, len(peers) + 1 + jnp.where(is_owner, members, 0))

    def place_of(half, n, sx, start, size):
        return xs.at[half, n // 4, pl.ds(pl.multiple_of(n % 4 * 128 + sx * UNIT, UNIT), UNIT), pl.ds(start, size)]

    def beside(p, owner):
        line = (owner[p] + 1 + 2 * (owner[p] % 2)) % 4
        return line, tuple(line if q == p else owner[q] for q in range(3))

    def detour(p, n, owner, source, sem):
        _, chip = beside(p, owner)
        slot = STEPS + n // 2
        copy = pltpu.make_async_remote_copy(
            source, relays[p].at[slot], sem, recv1.at[p, slot],
            device_id=device_at(*chip, core), device_id_type=MESH,
        )
        return jnp.logical_and(((x, y, z)[p] - owner[p] + 4) % 4 == 2, n % 2 == 1), copy

    def sends(n, wait):
        oy = (y - SKEW_Y * x - n // 4 + 16) % 4
        oz = (z - SKEW_Z * x - n % 4 + 16) % 4
        ox = (oy + oz) % 4
        to = class_at(oy, oz)
        for p, (start, size) in enumerate(PARTS):
            rx, ry, rz = ((x, oy, oz), (ox, y, oz), (ox, oy, z))[p]
            own = both_true(rx == x, ry == y, rz == z)
            last = both_true(rx == ox, ry == oy, rz == oz)
            source = out_ref.at[pl.ds(pl.multiple_of(to * UNIT, UNIT), UNIT), pl.ds(start, size)]
            dest = place_of(core, n, x, start, size)
            via = pltpu.make_async_remote_copy(
                source, relays[p].at[n], send1.at[p, n], recv1.at[p, n],
                device_id=device_at(rx, ry, rz, core), device_id_type=MESH,
            )
            direct = pltpu.make_async_remote_copy(
                source, dest, send1.at[p, n], rstep.at[n],
                device_id=device_at(ox, oy, oz, core), device_id_type=MESH,
            )
            here = jnp.logical_and(own, last)
            aside, bypass = detour(p, n, (ox, oy, oz), source, send1.at[p, n])
            aside = jnp.logical_and(own, aside)
            if wait:

                @pl.when(jnp.logical_not(here))
                def _():
                    direct.wait_send()

            else:

                @pl.when(jnp.logical_not(jnp.logical_or(own, last)))
                def _():
                    via.start()

                @pl.when(jnp.logical_and(jnp.logical_xor(own, last), jnp.logical_not(aside)))
                def _():
                    direct.start()

                @pl.when(aside)
                def _():
                    bypass.start()

    def line_owner(p):
        if p == 0:
            return (y + z) % 4, y, z
        if p == 1:
            return x, (x - z + 4) % 4, z
        return x, y, (x - y + 4) % 4

    def source_of(p, n, owner, line):
        _, oy, oz = owner
        if p == 0:
            sx = line
        elif p == 1:
            sx = (SKEW_Y * (line - oy - n // 4) + 16) % 4
        else:
            sx = (SKEW_Z * (line - oz - n % 4 + 8)) % 4
        return sx, (oy + SKEW_Y * sx + n // 4) % 4, (oz + SKEW_Z * sx + n % 4) % 4

    def pass_on(p, n, slot, owner, sx):
        start, size = PARTS[p]
        return pltpu.make_async_remote_copy(
            relays[p].at[slot], place_of(core, n, sx, start, size), send2.at[p, slot], rstep.at[n],
            device_id=device_at(*owner, core), device_id_type=MESH,
        )

    def arrived(p, slot):
        pltpu.make_async_copy(relays[p].at[slot], relays[p].at[slot], recv1.at[p, slot]).wait()

    def forwards(n, wait):
        for p in range(3):
            owner = line_owner(p)
            here = (x, y, z)[p]
            sx, sy, sz = source_of(p, n, owner, here)
            mine = both_true(sx == x, sy == y, sz == z)
            copy = pass_on(p, n, n, owner, sx)
            aside, bypass = detour(p, n, owner, relays[p].at[n], send2.at[p, n])

            @pl.when(jnp.logical_not(mine))
            def _():
                if wait:
                    copy.wait_send()
                else:
                    arrived(p, n)

                    @pl.when(aside)
                    def _():
                        bypass.start()

                    @pl.when(jnp.logical_not(aside))
                    def _():
                        copy.start()

            slot = STEPS + n // 2
            fx, _, _ = source_of(p, n, owner, (owner[p] + 2) % 4)
            far = pass_on(p, n, slot, owner, fx)

            @pl.when(jnp.logical_and(here == beside(p, owner)[0], n % 2 == 1))
            def _():
                if wait:
                    far.wait_send()
                else:
                    arrived(p, slot)
                    far.start()

    repeat(STEPS, lambda n: sends(n, False))

    @pl.when(jnp.logical_not(is_owner))
    def _():
        repeat(STEPS, lambda n: forwards(n, False))
        repeat(STEPS, lambda n: forwards(n, True))

    def tile(half, s, r, slot):
        gram[slot] = lax.dot_general(
            xs[half, s], xs[core, r], (((1,), (1,)), ((), ())), preferred_element_type=jnp.float32
        )

    def half_tile(half, s, h, slot):
        lines = pl.ds(pl.multiple_of(h * 256, 256), 256)
        gram[slot, :, lines] = lax.dot_general(
            xs[half, s], xs[core, 3, lines], (((1,), (1,)), ((), ())), preferred_element_type=jnp.float32
        )

    def across(r):
        return pltpu.make_async_remote_copy(
            xs.at[core, r], xs.at[core, r], dsend.at[r], drecv.at[r], device_id=partner, device_id_type=MESH
        )

    def across_half(h):
        rows = xs.at[core, 3, pl.ds(pl.multiple_of(h * 256, 256), 256)]
        return pltpu.make_async_remote_copy(
            rows, rows, dsend.at[3 + h], drecv.at[3 + h], device_id=partner, device_id_type=MESH
        )

    def share_copy(m):
        return pltpu.make_async_remote_copy(
            final.at[m], landed.at[core], msend.at[m], mrecv.at[core], device_id=(m, klass), device_id_type=MESH
        )

    @pl.when(is_owner)
    def _():
        self_step = (4 - SKEW_Y) * x % 4 * 4 + (4 - SKEW_Z) * x % 4
        xs[core, self_step // 4, pl.ds(pl.multiple_of(self_step % 4 * 128 + x * UNIT, UNIT), UNIT)] = xs[
            other, 0, pl.ds(pl.multiple_of(klass * UNIT, UNIT), UNIT)
        ]
        repeat(STEPS, lambda n: sends(n, True))
        pl.semaphore_signal(credit, inc=1, device_id=partner, device_id_type=MESH)
        pl.semaphore_wait(credit, 1)
        pacc[...] = jnp.zeros_like(pacc)

        def take(half, r):
            pacc[...] += jnp.dot(pick_ref[half, r], xs[half, r], preferred_element_type=jnp.float32)

        def steps_in(r, first, count):
            for q in range(count):
                n = r * 4 + first + q
                for mine, count in ((False, 128), (True, 128 - UNIT)):
                    rows = xs.at[core, r, pl.ds(pl.multiple_of((first + q) * 128, 128), count)]

                    @pl.when((n == self_step) == mine)
                    def _():
                        pltpu.make_async_copy(rows, rows, rstep.at[n]).wait()

        def other_in(r):
            across(r).wait_recv()
            take(other, r)

            @pl.when(r % 2 == core)
            def _():
                tile(other, r, r, 16 + r // 2)

        def round_of(r):
            steps_in(r, 0, 4)
            across(r).start()
            take(core, r)

            def own_tile(s, carry):
                tile(core, s, r, r * (r + 1) // 2 + s)
                return carry

            lax.fori_loop(0, r + 1, own_tile, 0)

            @pl.when(r > 0)
            def _():
                other_in(r - 1)

            def cross_tile(s, carry):
                tile(other, s, r, 10 + r * (r - 1) // 2 + s)
                return carry

            lax.fori_loop(0, r, cross_tile, 0)

        repeat(3, round_of)

        def last_half(h):
            steps_in(3, 2 * h, 2)
            across_half(h).start()
            repeat(3, lambda s: half_tile(core, s, h, 6 + s))

            @pl.when(h == 0)
            def _():
                other_in(2)

            repeat(3, lambda s: half_tile(other, s, h, 13 + s))

        repeat(2, last_half)
        take(core, 3)
        tile(core, 3, 3, 9)
        for h in range(2):
            across_half(h).wait_recv()
        take(other, 3)

        @pl.when(core == 1)
        def _():
            tile(other, 3, 3, 17)

        wide = pacc[...]
        mass = wide[3:4]
        high = mass.astype(jnp.bfloat16).astype(jnp.float32)
        middle = (mass - high).astype(jnp.bfloat16).astype(jnp.float32)
        line = lax.broadcasted_iota(jnp.int32, (EXT, D), 0)
        hp = [0.5 * jnp.sum(wide[t : t + 1] * wide[t : t + 1], axis=1, keepdims=True) for t in range(3)]
        wide = jnp.where(line == 3, high, jnp.where(line == 4, middle, jnp.where(line == 5, mass - high - middle, wide)))
        picked = wide.astype(jnp.bfloat16)

        eye = lax.broadcasted_iota(jnp.int32, (128, 128), 0) == lax.broadcasted_iota(jnp.int32, (128, 128), 1)

        def group(n, xx):
            ny = (y + SKEW_Y * xx + n // 4) % 4
            nz = (z + SKEW_Z * xx + n % 4) % 4
            return ny, nz

        lane = lax.broadcasted_iota(jnp.int32, (8, 128), 1) // UNIT

        def own_rows(r):
            near = lax.dot_general(
                picked, xs[core, r], (((1,), (1,)), ((), ())), preferred_element_type=jnp.float32
            )
            for q in range(4):
                n = r * 4 + q
                lanes = slice(q * 128, q * 128 + 128)
                sub = gram[r * (r + 3) // 2, lanes, lanes]
                h = 0.5 * jnp.sum(jnp.where(eye, sub, 0.0), axis=0, keepdims=True)
                good = jnp.zeros((8, 128), jnp.float32)
                for xx in range(4):
                    ny, nz = group(n, xx)
                    piece = jnp.broadcast_to(valid_ref[core * 16 + xx * 4 + ny], (8, 128))
                    good = jnp.where(lane == xx, pltpu.roll(piece, (xx - nz + 4) % 4 * UNIT, 1), good)
                ok = good[0:1] > 0.0
                p1 = hp[0] - near[0:1, lanes]
                p2 = jnp.minimum(p1, hp[1] - near[1:2, lanes])
                p3 = jnp.minimum(p2, hp[2] - near[2:3, lanes])
                tab[core, r, 0:1, lanes] = jnp.where(ok, h, -BIG)
                tab[core, r, 1:2, lanes] = jnp.where(ok, p1, -BIG)
                tab[core, r, 2:3, lanes] = jnp.where(ok, p2, -BIG)
                tab[core, r, 3:4, lanes] = p3
                tab[core, r, 4:5, lanes] = h
                tab[core, r, 5:6, lanes] = good[0:1]
                tab[core, r, 6:7, lanes] = near[3:4, lanes] + near[4:5, lanes] + near[5:6, lanes]

        repeat(4, own_rows)
        sums[...] = jnp.zeros_like(sums)
        peak[...] = jnp.zeros_like(peak)
        tables = pltpu.make_async_remote_copy(
            tab.at[core], tab.at[core], tsend.at[0], trecv.at[0], device_id=partner, device_id_type=MESH
        )

        def row_block(b):
            half = jnp.where(b < 4, core, other)
            s = b % 4
            mine = b < 4

            @pl.when(b == 1)
            def _():
                tables.start()

            @pl.when(b == 4)
            def _():
                tables.wait()

            hcol[...] = column(tab[half, s, 0:1])
            a1col[...] = column(tab[half, s, 1:2])
            a2col[...] = column(tab[half, s, 2:3])
            r1[...] = jnp.zeros_like(r1)
            r2[...] = jnp.zeros_like(r2)

            def one_tile(r, carry):
                slot = jnp.where(
                    mine, r * (r + 1) // 2 + s, jnp.where(r == s, 16 + s // 2, 10 + r * (r - 1) // 2 + s)
                )
                diag = jnp.logical_and(mine, r == s)

                def sweep(rows_too):
                    for cb in range(4):
                        lanes = slice(cb * 128, cb * 128 + 128)
                        hu = tab[core, r, 0:1, lanes]
                        a1u = tab[core, r, 1:2, lanes]
                        a2u = tab[core, r, 2:3, lanes]

                        def strip(k, acc):
                            c1, c2, low = acc
                            at = pl.ds(pl.multiple_of(k * 32, 32), 32)
                            g = gram[slot, at, lanes]
                            e = g - hu
                            f = g - hcol[at]
                            c1 = c1 + fold(jnp.maximum(e + a1col[at], 0.0))
                            c2 = c2 + fold(jnp.maximum(e + a2col[at], 0.0))
                            low = jnp.minimum(
                                low, jnp.minimum(jnp.minimum(f[0:8], f[8:16]), jnp.minimum(f[16:24], f[24:32]))
                            )
                            if rows_too:
                                r1[at] += jnp.maximum(f + a1u, 0.0)
                                r2[at] += jnp.maximum(f + a2u, 0.0)
                            return c1, c2, low

                        zero = jnp.zeros((8, 128), jnp.float32)
                        c1, c2, low = lax.fori_loop(0, BS // 32, strip, (zero, zero, zero + BIG), unroll=4)
                        sums[r, 0, :, lanes] += c1
                        sums[r, 1, :, lanes] += c2
                        peak[...] = jnp.maximum(peak[...], hu - low)

                @pl.when(diag)
                def _():
                    sweep(False)

                @pl.when(jnp.logical_not(diag))
                def _():
                    sweep(True)

                return carry

            begin = jnp.where(jnp.logical_or(mine, s % 2 == core), s, s + 1)
            lax.fori_loop(begin, 4, one_tile, 0)
            for n, acc in enumerate((r1, r2)):
                part[half, s, n : n + 1] = jnp.sum(acc[...].T, axis=0, keepdims=True)

        repeat(8, row_block)
        best = jnp.max(jnp.max(peak[...], axis=0, keepdims=True), axis=1, keepdims=True)
        for r in range(4):
            part[other, r, 3:4] = jnp.broadcast_to(best, (1, BS))
        partial = pltpu.make_async_remote_copy(
            part.at[other], got, tsend.at[1], trecv.at[1], device_id=partner, device_id_type=MESH
        )
        total = jnp.sum(jnp.sum(valid_ref[...], axis=0), axis=1, keepdims=True)
        h_sum = jnp.zeros((1, 1), jnp.float32)
        for half in range(2):
            for r in range(4):
                h_sum = h_sum + jnp.sum(tab[half, r, 4:5], axis=1, keepdims=True)
        partial.start()
        partial.wait()
        bound = jnp.maximum(best, got[0, 3:4, 0:1]) * SCALE

        for r in range(4):
            cols = [jnp.sum(sums[r, n], axis=0, keepdims=True) + part[core, r, n : n + 1] + got[r, n : n + 1] for n in range(2)]
            h = tab[core, r, 4:5]
            ok = tab[core, r, 5:6] > 0.0
            far = total * h + h_sum - tab[core, r, 6:7]
            part[core, r, 4:5] = jnp.where(ok, (total * bound - far * SCALE) / total, 0.0)
            part[core, r, 5:6] = jnp.where(ok, cols[0] * SCALE / total, 0.0)
            part[core, r, 6:7] = jnp.where(ok, cols[1] * SCALE / total, 0.0)
            part[core, r, 7:8] = jnp.where(ok, jnp.maximum(bound - (h + tab[core, r, 3:4]) * SCALE, 0.0), 0.0)

        def natural(n):
            xx, ny = n // 4, n % 4
            i1 = (ny - y - SKEW_Y * xx + 16) % 4
            piece = jnp.zeros((8, 128), jnp.float32)
            for nz in range(4):
                i2 = (nz - z - SKEW_Z * xx + 16) % 4
                take = part[core, i1, :, pl.ds(pl.multiple_of(i2 * 128, 128), 128)]
                piece = jnp.where(lane == nz, pltpu.roll(take, (nz - xx + 4) % 4 * UNIT, 1), piece)
            seat = lax.broadcasted_iota(jnp.int32, (8, 128), 1) % UNIT // 4 == 2 * ny + core
            for m in range(8):
                spot = pltpu.roll(piece, (2 * ny + core - m + 32) * 4 % 128, 1)
                final[m, :, pl.ds(pl.multiple_of(xx * 128, 128), 128)] += jnp.where(seat, spot, 0.0)[4:8]

        final[...] = jnp.zeros_like(final)
        lax.fori_loop(0, 16, lambda n, carry: (natural(n), carry)[1], 0, unroll=4)
        me = lax.axis_index("dp")
        for m in range(8):
            local = jnp.logical_and(me == m, cls == klass)

            @pl.when(jnp.logical_not(local))
            def _():
                share_copy(m).start()

            @pl.when(local)
            def _():
                landed[core] = final[m]

        for m in range(8):
            local = jnp.logical_and(me == m, cls == klass)

            @pl.when(jnp.logical_not(local))
            def _():
                share_copy(m).wait_send()

        repeat(3, lambda r: across(r).wait_send())
        repeat(2, lambda h: across_half(h).wait_send())

    @pl.when(jnp.logical_not(is_owner))
    def _():
        repeat(STEPS, lambda n: sends(n, True))

    for c in range(2):
        local = both_true(is_owner, core == c, cls == klass)

        @pl.when(jnp.logical_not(local))
        def _():
            pltpu.make_async_copy(landed.at[c], landed.at[c], mrecv.at[c]).wait()


def select_facilities(target, sketches, pick, valid):
    vmem = pl.BlockSpec(memory_space=pltpu.VMEM)
    sems = pltpu.SemaphoreType.DMA
    wide = pltpu.VMEM((BS, 128), jnp.float32)
    return pl.pallas_call(
        kernel,
        out_shape=jax.ShapeDtypeStruct((2, 4, BS), jnp.float32),
        in_specs=[vmem, pl.BlockSpec(memory_space=pl.ANY), vmem, vmem],
        out_specs=vmem,
        scratch_shapes=[pltpu.VMEM((2, 4, BS, D), jnp.bfloat16)]
        + [pltpu.VMEM((STEPS + STEPS // 2, UNIT, size), jnp.bfloat16) for _, size in PARTS]
        + [
            pltpu.VMEM((18, BS, BS), jnp.float32),
            pltpu.VMEM((2, 4, 8, BS), jnp.float32),
            wide, wide, wide, wide, wide,
            pltpu.VMEM((4, 2, 8, BS), jnp.float32),
            pltpu.VMEM((8, 128), jnp.float32),
            pltpu.VMEM((2, 4, 8, BS), jnp.float32),
            pltpu.VMEM((4, 8, BS), jnp.float32),
            pltpu.VMEM((8, 4, BS), jnp.float32),
            pltpu.VMEM((EXT, D), jnp.float32),
            sems((3, STEPS)), sems((3, STEPS + STEPS // 2)), sems((3, STEPS + STEPS // 2)), sems((STEPS,)),
            sems((5,)), sems((5,)), sems((2,)), sems((2,)), sems((8,)), sems((2,)),
            sems, pltpu.SemaphoreType.REGULAR,
        ],
        compiler_params=pltpu.CompilerParams(collective_id=0, has_side_effects=True, vmem_limit_bytes=62 * 1024 * 1024),
        name="facilities",
    )(target, sketches, pick, valid)


def body(sketches, labels, places, counts, chosen):
    member = lax.axis_index("dp")
    cls = lax.axis_index("cls")
    info = jnp.concatenate([counts[0], jnp.pad(chosen[:, :1], ((0, 5), (0, 127)))], axis=0)
    swapped = lax.ppermute(info, "cls", [(n, n ^ 1) for n in range(16)])
    target = labels * UNIT + places // 512 * 4 + places % 4

    x, y, z, core = member // 2, (cls // 2) % 4, (member % 2) * 2 + cls // 8, cls % 2
    info = jnp.where(core == z // 2, info, swapped)
    picked = info[8:11, 0]
    source = picked % 512 // 4
    sx, sz, sy, score = source // 32, source // 8 % 4, source // 2 % 4, source % 2
    step = (sy - y - SKEW_Y * sx + 16) % 4 * 4 + (sz - z - SKEW_Z * sx + 16) % 4
    where = score * HALF + step * 128 + sx * UNIT + picked // 512 * 4 + picked % 4
    spot = jnp.pad(where, (0, EXT - 3), constant_values=-1)
    line = jnp.arange(4096, dtype=jnp.int32).reshape(8, 1, BS)
    everyone = jnp.arange(EXT, dtype=jnp.int32)[None, :, None] == 3
    pick = ((line == spot[None, :, None]) | everyone).astype(jnp.bfloat16).reshape(2, 4, EXT, BS)
    by_source = jnp.transpose(info[:8].reshape(8, 4, 4, 4, 2), (4, 1, 3, 2, 0))
    valid = (jnp.arange(4, dtype=jnp.int32) < by_source[..., None]).astype(jnp.float32).reshape(32, 1, 128)

    both = select_facilities(target[None, :], sketches, pick, valid)
    return (both[0, :3, None, :] + both[1, :3, None, :], both[0, 3:] + both[1, 3:])


def solution(mesh):
    placed = (
        P(("dp", "cls"), None),
        P(("dp", "cls")),
        P(("dp", "cls")),
        P("cls", None, None),
        P(None, "cls"),
    )
    return jax.shard_map(
        body,
        mesh=mesh,
        in_specs=placed,
        out_specs=(P(None, "cls", "dp"), P("cls", "dp")),
        check_vma=False,
    )
```

```python
import jax
import jax.numpy as jnp
from jax import lax
from jax.experimental import pallas as pl
from jax.experimental.pallas import tpu as pltpu
from jax.sharding import PartitionSpec as P

MESH = pl.DeviceIdType.MESH
D = 4096
BIG = 1e30
SCALE = 2.0 / D
PARTS = ((0, 1280), (1280, 1408), (2688, 1408))
UNIT = 32
STEPS = 16
BS = 512
HALF = 2048
EXT = 16
SKEW_Y = 1
SKEW_Z = 3


def my_coords():
    dp = lax.axis_index("dp")
    cls = lax.axis_index("cls")
    return dp // 2, (cls // 2) % 4, (dp % 2) * 2 + cls // 8, cls % 2


def device_at(x, y, z, core):
    return (x * 2 + z // 2, ((z % 2) * 4 + y) * 2 + core)


def class_at(y, z):
    return (z % 2) * 8 + y * 2 + z // 2


def both_true(a, b, c):
    return jnp.logical_and(jnp.logical_and(a, b), c)


def repeat(count, step):
    def once(n, carry):
        step(n)
        return carry

    lax.fori_loop(0, count, once, 0)


def column(row):
    return jnp.broadcast_to(row, (128, row.shape[1])).T


def fold(v):
    return (v[0:8] + v[8:16]) + (v[16:24] + v[24:32])


def kernel(target_ref, sketch_ref, pick_ref, valid_ref, landed, xs, relay0, relay1, relay2, gram, tab, hcol, a1col, a2col,
           r1, r2, sums, peak, part, got, final, pacc, send1, recv1, send2, rstep, dsend, drecv, tsend, trecv, msend, mrecv, load_sem, credit):
    x, y, z, core = my_coords()
    relays = (relay0, relay1, relay2)
    is_owner = x == (y + z) % 4
    partner = device_at(x, y, z, 1 - core)
    klass = class_at(y, z)
    cls = lax.axis_index("cls")
    other = 1 - core
    out_ref = xs.at[other, 0]
    load = pltpu.make_async_copy(sketch_ref, xs.at[other, 1, pl.ds(0, 256)], load_sem)
    load.start()

    barrier = pltpu.get_barrier_semaphore()

    def greet(who):
        pl.semaphore_signal(barrier, inc=1, device_id=who, device_id_type=MESH)

    peers = [(a, b, c) for a in range(4) for b in range(4) for c in range(4) if 0 in (a, b, c) and (a, b, c) != (0, 0, 0)]
    for a, b, c in peers:
        greet(device_at((x + a) % 4, (y + b) % 4, (z + c) % 4, core))
    greet(partner)
    home_z = 2 * (cls % 2) + cls // 8
    home_x = (y + home_z) % 4
    for c in range(2):

        @pl.when(jnp.logical_not(both_true(home_x == x, home_z == z, core == c)))
        def _():
            greet(device_at(home_x, y, home_z, c))

    load.wait()
    table = (lax.broadcasted_iota(jnp.int32, (512, 256), 0) == target_ref[...]).astype(jnp.bfloat16)

    def place_slots(n):
        lanes = pl.ds(pl.multiple_of(n * 512, 512), 512)
        xs[other, 0, :, lanes] = jnp.dot(
            table, xs[other, 1, 0:256, lanes], preferred_element_type=jnp.float32
        ).astype(jnp.bfloat16)

    repeat(8, place_slots)
    members = jnp.where(cls == klass, 7, 8)
    pl.semaphore_wait(barrier, len(peers) + 1 + jnp.where(is_owner, members, 0))

    def place_of(half, n, sx, start, size):
        return xs.at[half, n // 4, pl.ds(pl.multiple_of(n % 4 * 128 + sx * UNIT, UNIT), UNIT), pl.ds(start, size)]

    def beside(p, owner):
        line = (owner[p] + 1 + 2 * (owner[p] % 2)) % 4
        return line, tuple(line if q == p else owner[q] for q in range(3))

    def detour(p, n, owner, source, sem):
        _, chip = beside(p, owner)
        slot = STEPS + n // 2
        copy = pltpu.make_async_remote_copy(
            source, relays[p].at[slot], sem, recv1.at[p, slot],
            device_id=device_at(*chip, core), device_id_type=MESH,
        )
        return jnp.logical_and(((x, y, z)[p] - owner[p] + 4) % 4 == 2, n % 2 == 1), copy

    def sends(n, wait):
        oy = (y - SKEW_Y * x - n // 4 + 16) % 4
        oz = (z - SKEW_Z * x - n % 4 + 16) % 4
        ox = (oy + oz) % 4
        to = class_at(oy, oz)
        for p, (start, size) in enumerate(PARTS):
            rx, ry, rz = ((x, oy, oz), (ox, y, oz), (ox, oy, z))[p]
            own = both_true(rx == x, ry == y, rz == z)
            last = both_true(rx == ox, ry == oy, rz == oz)
            source = out_ref.at[pl.ds(pl.multiple_of(to * UNIT, UNIT), UNIT), pl.ds(start, size)]
            dest = place_of(core, n, x, start, size)
            via = pltpu.make_async_remote_copy(
                source, relays[p].at[n], send1.at[p, n], recv1.at[p, n],
                device_id=device_at(rx, ry, rz, core), device_id_type=MESH,
            )
            direct = pltpu.make_async_remote_copy(
                source, dest, send1.at[p, n], rstep.at[n],
                device_id=device_at(ox, oy, oz, core), device_id_type=MESH,
            )
            here = jnp.logical_and(own, last)
            aside, bypass = detour(p, n, (ox, oy, oz), source, send1.at[p, n])
            aside = jnp.logical_and(own, aside)
            if wait:

                @pl.when(jnp.logical_not(here))
                def _():
                    direct.wait_send()

            else:

                @pl.when(jnp.logical_not(jnp.logical_or(own, last)))
                def _():
                    via.start()

                @pl.when(jnp.logical_and(jnp.logical_xor(own, last), jnp.logical_not(aside)))
                def _():
                    direct.start()

                @pl.when(aside)
                def _():
                    bypass.start()

    def line_owner(p):
        if p == 0:
            return (y + z) % 4, y, z
        if p == 1:
            return x, (x - z + 4) % 4, z
        return x, y, (x - y + 4) % 4

    def source_of(p, n, owner, line):
        _, oy, oz = owner
        if p == 0:
            sx = line
        elif p == 1:
            sx = (SKEW_Y * (line - oy - n // 4) + 16) % 4
        else:
            sx = (SKEW_Z * (line - oz - n % 4 + 8)) % 4
        return sx, (oy + SKEW_Y * sx + n // 4) % 4, (oz + SKEW_Z * sx + n % 4) % 4

    def pass_on(p, n, slot, owner, sx):
        start, size = PARTS[p]
        return pltpu.make_async_remote_copy(
            relays[p].at[slot], place_of(core, n, sx, start, size), send2.at[p, slot], rstep.at[n],
            device_id=device_at(*owner, core), device_id_type=MESH,
        )

    def arrived(p, slot):
        pltpu.make_async_copy(relays[p].at[slot], relays[p].at[slot], recv1.at[p, slot]).wait()

    def forwards(n, wait):
        for p in range(3):
            owner = line_owner(p)
            here = (x, y, z)[p]
            sx, sy, sz = source_of(p, n, owner, here)
            mine = both_true(sx == x, sy == y, sz == z)
            copy = pass_on(p, n, n, owner, sx)
            aside, bypass = detour(p, n, owner, relays[p].at[n], send2.at[p, n])

            @pl.when(jnp.logical_not(mine))
            def _():
                if wait:
                    copy.wait_send()
                else:
                    arrived(p, n)

                    @pl.when(aside)
                    def _():
                        bypass.start()

                    @pl.when(jnp.logical_not(aside))
                    def _():
                        copy.start()

            slot = STEPS + n // 2
            fx, _, _ = source_of(p, n, owner, (owner[p] + 2) % 4)
            far = pass_on(p, n, slot, owner, fx)

            @pl.when(jnp.logical_and(here == beside(p, owner)[0], n % 2 == 1))
            def _():
                if wait:
                    far.wait_send()
                else:
                    arrived(p, slot)
                    far.start()

    repeat(STEPS, lambda n: sends(n, False))

    @pl.when(jnp.logical_not(is_owner))
    def _():
        repeat(STEPS, lambda n: forwards(n, False))
        repeat(STEPS, lambda n: forwards(n, True))

    def tile(half, s, r, slot):
        gram[slot] = lax.dot_general(
            xs[half, s], xs[core, r], (((1,), (1,)), ((), ())), preferred_element_type=jnp.float32
        )

    def half_tile(half, s, h, slot):
        lines = pl.ds(pl.multiple_of(h * 256, 256), 256)
        gram[slot, :, lines] = lax.dot_general(
            xs[half, s], xs[core, 3, lines], (((1,), (1,)), ((), ())), preferred_element_type=jnp.float32
        )

    def across(r):
        return pltpu.make_async_remote_copy(
            xs.at[core, r], xs.at[core, r], dsend.at[r], drecv.at[r], device_id=partner, device_id_type=MESH
        )

    def across_half(h):
        rows = xs.at[core, 3, pl.ds(pl.multiple_of(h * 256, 256), 256)]
        return pltpu.make_async_remote_copy(
            rows, rows, dsend.at[3 + h], drecv.at[3 + h], device_id=partner, device_id_type=MESH
        )

    def share_copy(m):
        return pltpu.make_async_remote_copy(
            final.at[m], landed.at[core], msend.at[m], mrecv.at[core], device_id=(m, klass), device_id_type=MESH
        )

    @pl.when(is_owner)
    def _():
        self_step = (4 - SKEW_Y) * x % 4 * 4 + (4 - SKEW_Z) * x % 4
        xs[core, self_step // 4, pl.ds(pl.multiple_of(self_step % 4 * 128 + x * UNIT, UNIT), UNIT)] = xs[
            other, 0, pl.ds(pl.multiple_of(klass * UNIT, UNIT), UNIT)
        ]
        repeat(STEPS, lambda n: sends(n, True))
        pl.semaphore_signal(credit, inc=1, device_id=partner, device_id_type=MESH)
        pl.semaphore_wait(credit, 1)
        pacc[...] = jnp.zeros_like(pacc)

        def take(half, r):
            pacc[...] += jnp.dot(pick_ref[half, r], xs[half, r], preferred_element_type=jnp.float32)

        def steps_in(r, first, count):
            for q in range(count):
                n = r * 4 + first + q
                for mine, count in ((False, 128), (True, 128 - UNIT)):
                    rows = xs.at[core, r, pl.ds(pl.multiple_of((first + q) * 128, 128), count)]

                    @pl.when((n == self_step) == mine)
                    def _():
                        pltpu.make_async_copy(rows, rows, rstep.at[n]).wait()

        def other_in(r):
            across(r).wait_recv()
            take(other, r)

            @pl.when(r % 2 == core)
            def _():
                tile(other, r, r, 16 + r // 2)

        def round_of(r):
            steps_in(r, 0, 4)
            across(r).start()
            take(core, r)

            def own_tile(s, carry):
                tile(core, s, r, r * (r + 1) // 2 + s)
                return carry

            lax.fori_loop(0, r + 1, own_tile, 0)

            @pl.when(r > 0)
            def _():
                other_in(r - 1)

            def cross_tile(s, carry):
                tile(other, s, r, 10 + r * (r - 1) // 2 + s)
                return carry

            lax.fori_loop(0, r, cross_tile, 0)

        repeat(3, round_of)

        def last_half(h):
            steps_in(3, 2 * h, 2)
            across_half(h).start()
            repeat(3, lambda s: half_tile(core, s, h, 6 + s))

            @pl.when(h == 0)
            def _():
                other_in(2)

            repeat(3, lambda s: half_tile(other, s, h, 13 + s))

        repeat(2, last_half)
        take(core, 3)
        tile(core, 3, 3, 9)
        for h in range(2):
            across_half(h).wait_recv()
        take(other, 3)

        @pl.when(core == 1)
        def _():
            tile(other, 3, 3, 17)

        wide = pacc[...]
        mass = wide[3:4]
        high = mass.astype(jnp.bfloat16).astype(jnp.float32)
        middle = (mass - high).astype(jnp.bfloat16).astype(jnp.float32)
        line = lax.broadcasted_iota(jnp.int32, (EXT, D), 0)
        hp = [0.5 * jnp.sum(wide[t : t + 1] * wide[t : t + 1], axis=1, keepdims=True) for t in range(3)]
        wide = jnp.where(line == 3, high, jnp.where(line == 4, middle, jnp.where(line == 5, mass - high - middle, wide)))
        picked = wide.astype(jnp.bfloat16)

        eye = lax.broadcasted_iota(jnp.int32, (128, 128), 0) == lax.broadcasted_iota(jnp.int32, (128, 128), 1)

        def group(n, xx):
            ny = (y + SKEW_Y * xx + n // 4) % 4
            nz = (z + SKEW_Z * xx + n % 4) % 4
            return ny, nz

        lane = lax.broadcasted_iota(jnp.int32, (8, 128), 1) // UNIT

        def own_rows(r):
            near = lax.dot_general(
                picked, xs[core, r], (((1,), (1,)), ((), ())), preferred_element_type=jnp.float32
            )
            for q in range(4):
                n = r * 4 + q
                lanes = slice(q * 128, q * 128 + 128)
                sub = gram[r * (r + 3) // 2, lanes, lanes]
                h = 0.5 * jnp.sum(jnp.where(eye, sub, 0.0), axis=0, keepdims=True)
                good = jnp.zeros((8, 128), jnp.float32)
                for xx in range(4):
                    ny, nz = group(n, xx)
                    piece = jnp.broadcast_to(valid_ref[core * 16 + xx * 4 + ny], (8, 128))
                    good = jnp.where(lane == xx, pltpu.roll(piece, (xx - nz + 4) % 4 * UNIT, 1), good)
                ok = good[0:1] > 0.0
                p1 = hp[0] - near[0:1, lanes]
                p2 = jnp.minimum(p1, hp[1] - near[1:2, lanes])
                p3 = jnp.minimum(p2, hp[2] - near[2:3, lanes])
                tab[core, r, 0:1, lanes] = jnp.where(ok, h, -BIG)
                tab[core, r, 1:2, lanes] = jnp.where(ok, p1, -BIG)
                tab[core, r, 2:3, lanes] = jnp.where(ok, p2, -BIG)
                tab[core, r, 3:4, lanes] = p3
                tab[core, r, 4:5, lanes] = h
                tab[core, r, 5:6, lanes] = good[0:1]
                tab[core, r, 6:7, lanes] = near[3:4, lanes] + near[4:5, lanes] + near[5:6, lanes]

        repeat(4, own_rows)
        sums[...] = jnp.zeros_like(sums)
        peak[...] = jnp.zeros_like(peak)
        tables = pltpu.make_async_remote_copy(
            tab.at[core], tab.at[core], tsend.at[0], trecv.at[0], device_id=partner, device_id_type=MESH
        )

        def row_block(b):
            half = jnp.where(b < 4, core, other)
            s = b % 4
            mine = b < 4

            @pl.when(b == 1)
            def _():
                tables.start()

            @pl.when(b == 4)
            def _():
                tables.wait()

            hcol[...] = column(tab[half, s, 0:1])
            a1col[...] = column(tab[half, s, 1:2])
            a2col[...] = column(tab[half, s, 2:3])
            r1[...] = jnp.zeros_like(r1)
            r2[...] = jnp.zeros_like(r2)

            def one_tile(r, carry):
                slot = jnp.where(
                    mine, r * (r + 1) // 2 + s, jnp.where(r == s, 16 + s // 2, 10 + r * (r - 1) // 2 + s)
                )
                diag = jnp.logical_and(mine, r == s)

                def sweep(rows_too):
                    for cb in range(4):
                        lanes = slice(cb * 128, cb * 128 + 128)
                        hu = tab[core, r, 0:1, lanes]
                        a1u = tab[core, r, 1:2, lanes]
                        a2u = tab[core, r, 2:3, lanes]

                        def strip(k, acc):
                            c1, c2, low = acc
                            at = pl.ds(pl.multiple_of(k * 32, 32), 32)
                            g = gram[slot, at, lanes]
                            e = g - hu
                            f = g - hcol[at]
                            c1 = c1 + fold(jnp.maximum(e + a1col[at], 0.0))
                            c2 = c2 + fold(jnp.maximum(e + a2col[at], 0.0))
                            low = jnp.minimum(
                                low, jnp.minimum(jnp.minimum(f[0:8], f[8:16]), jnp.minimum(f[16:24], f[24:32]))
                            )
                            if rows_too:
                                r1[at] += jnp.maximum(f + a1u, 0.0)
                                r2[at] += jnp.maximum(f + a2u, 0.0)
                            return c1, c2, low

                        zero = jnp.zeros((8, 128), jnp.float32)
                        c1, c2, low = lax.fori_loop(0, BS // 32, strip, (zero, zero, zero + BIG), unroll=8)
                        sums[r, 0, :, lanes] += c1
                        sums[r, 1, :, lanes] += c2
                        peak[...] = jnp.maximum(peak[...], hu - low)

                @pl.when(diag)
                def _():
                    sweep(False)

                @pl.when(jnp.logical_not(diag))
                def _():
                    sweep(True)

                return carry

            begin = jnp.where(jnp.logical_or(mine, s % 2 == core), s, s + 1)
            lax.fori_loop(begin, 4, one_tile, 0)
            for n, acc in enumerate((r1, r2)):
                part[half, s, n : n + 1] = jnp.sum(acc[...].T, axis=0, keepdims=True)

        repeat(8, row_block)
        best = jnp.max(jnp.max(peak[...], axis=0, keepdims=True), axis=1, keepdims=True)
        for r in range(4):
            part[other, r, 3:4] = jnp.broadcast_to(best, (1, BS))
        partial = pltpu.make_async_remote_copy(
            part.at[other], got, tsend.at[1], trecv.at[1], device_id=partner, device_id_type=MESH
        )
        total = jnp.sum(jnp.sum(valid_ref[...], axis=0), axis=1, keepdims=True)
        h_sum = jnp.zeros((1, 1), jnp.float32)
        for half in range(2):
            for r in range(4):
                h_sum = h_sum + jnp.sum(tab[half, r, 4:5], axis=1, keepdims=True)
        partial.start()
        partial.wait()
        bound = jnp.maximum(best, got[0, 3:4, 0:1]) * SCALE

        for r in range(4):
            cols = [jnp.sum(sums[r, n], axis=0, keepdims=True) + part[core, r, n : n + 1] + got[r, n : n + 1] for n in range(2)]
            h = tab[core, r, 4:5]
            ok = tab[core, r, 5:6] > 0.0
            far = total * h + h_sum - tab[core, r, 6:7]
            part[core, r, 4:5] = jnp.where(ok, (total * bound - far * SCALE) / total, 0.0)
            part[core, r, 5:6] = jnp.where(ok, cols[0] * SCALE / total, 0.0)
            part[core, r, 6:7] = jnp.where(ok, cols[1] * SCALE / total, 0.0)
            part[core, r, 7:8] = jnp.where(ok, jnp.maximum(bound - (h + tab[core, r, 3:4]) * SCALE, 0.0), 0.0)

        def natural(n):
            xx, ny = n // 4, n % 4
            i1 = (ny - y - SKEW_Y * xx + 16) % 4
            piece = jnp.zeros((8, 128), jnp.float32)
            for nz in range(4):
                i2 = (nz - z - SKEW_Z * xx + 16) % 4
                take = part[core, i1, :, pl.ds(pl.multiple_of(i2 * 128, 128), 128)]
                piece = jnp.where(lane == nz, pltpu.roll(take, (nz - xx + 4) % 4 * UNIT, 1), piece)
            seat = lax.broadcasted_iota(jnp.int32, (8, 128), 1) % UNIT // 4 == 2 * ny + core
            for m in range(8):
                spot = pltpu.roll(piece, (2 * ny + core - m + 32) * 4 % 128, 1)
                final[m, :, pl.ds(pl.multiple_of(xx * 128, 128), 128)] += jnp.where(seat, spot, 0.0)[4:8]

        final[...] = jnp.zeros_like(final)
        lax.fori_loop(0, 16, lambda n, carry: (natural(n), carry)[1], 0, unroll=8)
        me = lax.axis_index("dp")
        for m in range(8):
            local = jnp.logical_and(me == m, cls == klass)

            @pl.when(jnp.logical_not(local))
            def _():
                share_copy(m).start()

            @pl.when(local)
            def _():
                landed[core] = final[m]

        for m in range(8):
            local = jnp.logical_and(me == m, cls == klass)

            @pl.when(jnp.logical_not(local))
            def _():
                share_copy(m).wait_send()

        repeat(3, lambda r: across(r).wait_send())
        repeat(2, lambda h: across_half(h).wait_send())

    @pl.when(jnp.logical_not(is_owner))
    def _():
        repeat(STEPS, lambda n: sends(n, True))

    for c in range(2):
        local = both_true(is_owner, core == c, cls == klass)

        @pl.when(jnp.logical_not(local))
        def _():
            pltpu.make_async_copy(landed.at[c], landed.at[c], mrecv.at[c]).wait()


def select_facilities(target, sketches, pick, valid):
    vmem = pl.BlockSpec(memory_space=pltpu.VMEM)
    sems = pltpu.SemaphoreType.DMA
    wide = pltpu.VMEM((BS, 128), jnp.float32)
    return pl.pallas_call(
        kernel,
        out_shape=jax.ShapeDtypeStruct((2, 4, BS), jnp.float32),
        in_specs=[vmem, pl.BlockSpec(memory_space=pl.ANY), vmem, vmem],
        out_specs=vmem,
        scratch_shapes=[pltpu.VMEM((2, 4, BS, D), jnp.bfloat16)]
        + [pltpu.VMEM((STEPS + STEPS // 2, UNIT, size), jnp.bfloat16) for _, size in PARTS]
        + [
            pltpu.VMEM((18, BS, BS), jnp.float32),
            pltpu.VMEM((2, 4, 8, BS), jnp.float32),
            wide, wide, wide, wide, wide,
            pltpu.VMEM((4, 2, 8, BS), jnp.float32),
            pltpu.VMEM((8, 128), jnp.float32),
            pltpu.VMEM((2, 4, 8, BS), jnp.float32),
            pltpu.VMEM((4, 8, BS), jnp.float32),
            pltpu.VMEM((8, 4, BS), jnp.float32),
            pltpu.VMEM((EXT, D), jnp.float32),
            sems((3, STEPS)), sems((3, STEPS + STEPS // 2)), sems((3, STEPS + STEPS // 2)), sems((STEPS,)),
            sems((5,)), sems((5,)), sems((2,)), sems((2,)), sems((8,)), sems((2,)),
            sems, pltpu.SemaphoreType.REGULAR,
        ],
        compiler_params=pltpu.CompilerParams(collective_id=0, has_side_effects=True, vmem_limit_bytes=62 * 1024 * 1024),
        name="facilities",
    )(target, sketches, pick, valid)


def body(sketches, labels, places, counts, chosen):
    member = lax.axis_index("dp")
    cls = lax.axis_index("cls")
    pairs = [(n, n ^ 1) for n in range(16)]
    counts_there = lax.ppermute(counts, "cls", pairs)
    chosen_there = lax.ppermute(chosen, "cls", pairs)
    target = labels * UNIT + places // 512 * 4 + places % 4

    x, y, z, core = member // 2, (cls // 2) % 4, (member % 2) * 2 + cls // 8, cls % 2
    ours = core == z // 2
    picked = jnp.where(ours, chosen, chosen_there)[:, 0]
    class_counts = jnp.where(ours, counts, counts_there)[0]
    source = picked % 512 // 4
    sx, sz, sy, score = source // 32, source // 8 % 4, source // 2 % 4, source % 2
    step = (sy - y - SKEW_Y * sx + 16) % 4 * 4 + (sz - z - SKEW_Z * sx + 16) % 4
    where = score * HALF + step * 128 + sx * UNIT + picked // 512 * 4 + picked % 4
    spot = jnp.pad(where, (0, EXT - 3), constant_values=-1)
    line = jnp.arange(4096, dtype=jnp.int32).reshape(8, 1, BS)
    everyone = jnp.arange(EXT, dtype=jnp.int32)[None, :, None] == 3
    pick = ((line == spot[None, :, None]) | everyone).astype(jnp.bfloat16).reshape(2, 4, EXT, BS)
    by_source = jnp.transpose(class_counts.reshape(8, 4, 4, 4, 2), (4, 1, 3, 2, 0))
    valid = (jnp.arange(4, dtype=jnp.int32) < by_source[..., None]).astype(jnp.float32).reshape(32, 1, 128)

    both = select_facilities(target[None, :], sketches, pick, valid)
    return (both[0, :3, None, :] + both[1, :3, None, :], both[0, 3:] + both[1, 3:])


def solution(mesh):
    placed = (
        P(("dp", "cls"), None),
        P(("dp", "cls")),
        P(("dp", "cls")),
        P("cls", None, None),
        P(None, "cls"),
    )
    return jax.shard_map(
        body,
        mesh=mesh,
        in_specs=placed,
        out_specs=(P(None, "cls", "dp"), P("cls", "dp")),
        check_vma=False,
    )
```

```python
import jax
import jax.numpy as jnp
from jax import lax
from jax.experimental import pallas as pl
from jax.experimental.pallas import tpu as pltpu
from jax.sharding import PartitionSpec as P

MESH = pl.DeviceIdType.MESH
D = 4096
BIG = 1e30
SCALE = 2.0 / D
PARTS = ((0, 1280), (1280, 1408), (2688, 1408))
UNIT = 32
STEPS = 16
BS = 512
HALF = 2048
EXT = 16
SKEW_Y = 1
SKEW_Z = 3


def my_coords():
    dp = lax.axis_index("dp")
    cls = lax.axis_index("cls")
    return dp // 2, (cls // 2) % 4, (dp % 2) * 2 + cls // 8, cls % 2


def device_at(x, y, z, core):
    return (x * 2 + z // 2, ((z % 2) * 4 + y) * 2 + core)


def class_at(y, z):
    return (z % 2) * 8 + y * 2 + z // 2


def both_true(a, b, c):
    return jnp.logical_and(jnp.logical_and(a, b), c)


def repeat(count, step):
    def once(n, carry):
        step(n)
        return carry

    lax.fori_loop(0, count, once, 0)


def column(row):
    return jnp.broadcast_to(row, (128, row.shape[1])).T


def fold(v):
    return (v[0:8] + v[8:16]) + (v[16:24] + v[24:32])


def kernel(target_ref, sketch_ref, pick_ref, valid_ref, landed, xs, relay0, relay1, relay2, gram, tab, hcol, a1col, a2col,
           r1, r2, sums, peak, part, got, final, pacc, send1, recv1, send2, rstep, dsend, drecv, tsend, trecv, msend, mrecv, load_sem, credit):
    x, y, z, core = my_coords()
    relays = (relay0, relay1, relay2)
    is_owner = x == (y + z) % 4
    partner = device_at(x, y, z, 1 - core)
    klass = class_at(y, z)
    cls = lax.axis_index("cls")
    other = 1 - core
    out_ref = xs.at[other, 0]
    load = pltpu.make_async_copy(sketch_ref, xs.at[other, 1, pl.ds(0, 256)], load_sem)
    load.start()

    barrier = pltpu.get_barrier_semaphore()

    def greet(who):
        pl.semaphore_signal(barrier, inc=1, device_id=who, device_id_type=MESH)

    peers = [(a, b, c) for a in range(4) for b in range(4) for c in range(4) if 0 in (a, b, c) and (a, b, c) != (0, 0, 0)]
    for a, b, c in peers:
        greet(device_at((x + a) % 4, (y + b) % 4, (z + c) % 4, core))
    greet(partner)
    home_z = 2 * (cls % 2) + cls // 8
    home_x = (y + home_z) % 4
    for c in range(2):

        @pl.when(jnp.logical_not(both_true(home_x == x, home_z == z, core == c)))
        def _():
            greet(device_at(home_x, y, home_z, c))

    load.wait()
    table = (lax.broadcasted_iota(jnp.int32, (512, 256), 0) == target_ref[...]).astype(jnp.bfloat16)

    def place_slots(n):
        lanes = pl.ds(pl.multiple_of(n * 512, 512), 512)
        xs[other, 0, :, lanes] = jnp.dot(
            table, xs[other, 1, 0:256, lanes], preferred_element_type=jnp.float32
        ).astype(jnp.bfloat16)

    repeat(8, place_slots)
    members = jnp.where(cls == klass, 7, 8)
    pl.semaphore_wait(barrier, len(peers) + 1 + jnp.where(is_owner, members, 0))

    def place_of(half, n, sx, start, size):
        return xs.at[half, n // 4, pl.ds(pl.multiple_of(n % 4 * 128 + sx * UNIT, UNIT), UNIT), pl.ds(start, size)]

    def beside(p, owner):
        line = (owner[p] + 1 + 2 * (owner[p] % 2)) % 4
        return line, tuple(line if q == p else owner[q] for q in range(3))

    def detour(p, n, owner, source, sem):
        _, chip = beside(p, owner)
        slot = STEPS + n // 2
        copy = pltpu.make_async_remote_copy(
            source, relays[p].at[slot], sem, recv1.at[p, slot],
            device_id=device_at(*chip, core), device_id_type=MESH,
        )
        return jnp.logical_and(((x, y, z)[p] - owner[p] + 4) % 4 == 2, n % 2 == 1), copy

    def sends(n, wait):
        oy = (y - SKEW_Y * x - n // 4 + 16) % 4
        oz = (z - SKEW_Z * x - n % 4 + 16) % 4
        ox = (oy + oz) % 4
        to = class_at(oy, oz)
        for p, (start, size) in enumerate(PARTS):
            rx, ry, rz = ((x, oy, oz), (ox, y, oz), (ox, oy, z))[p]
            own = both_true(rx == x, ry == y, rz == z)
            last = both_true(rx == ox, ry == oy, rz == oz)
            source = out_ref.at[pl.ds(pl.multiple_of(to * UNIT, UNIT), UNIT), pl.ds(start, size)]
            dest = place_of(core, n, x, start, size)
            via = pltpu.make_async_remote_copy(
                source, relays[p].at[n], send1.at[p, n], recv1.at[p, n],
                device_id=device_at(rx, ry, rz, core), device_id_type=MESH,
            )
            direct = pltpu.make_async_remote_copy(
                source, dest, send1.at[p, n], rstep.at[n],
                device_id=device_at(ox, oy, oz, core), device_id_type=MESH,
            )
            here = jnp.logical_and(own, last)
            aside, bypass = detour(p, n, (ox, oy, oz), source, send1.at[p, n])
            aside = jnp.logical_and(own, aside)
            if wait:

                @pl.when(jnp.logical_not(here))
                def _():
                    direct.wait_send()

            else:

                @pl.when(jnp.logical_not(jnp.logical_or(own, last)))
                def _():
                    via.start()

                @pl.when(jnp.logical_and(jnp.logical_xor(own, last), jnp.logical_not(aside)))
                def _():
                    direct.start()

                @pl.when(aside)
                def _():
                    bypass.start()

    def line_owner(p):
        if p == 0:
            return (y + z) % 4, y, z
        if p == 1:
            return x, (x - z + 4) % 4, z
        return x, y, (x - y + 4) % 4

    def source_of(p, n, owner, line):
        _, oy, oz = owner
        if p == 0:
            sx = line
        elif p == 1:
            sx = (SKEW_Y * (line - oy - n // 4) + 16) % 4
        else:
            sx = (SKEW_Z * (line - oz - n % 4 + 8)) % 4
        return sx, (oy + SKEW_Y * sx + n // 4) % 4, (oz + SKEW_Z * sx + n % 4) % 4

    def pass_on(p, n, slot, owner, sx):
        start, size = PARTS[p]
        return pltpu.make_async_remote_copy(
            relays[p].at[slot], place_of(core, n, sx, start, size), send2.at[p, slot], rstep.at[n],
            device_id=device_at(*owner, core), device_id_type=MESH,
        )

    def arrived(p, slot):
        pltpu.make_async_copy(relays[p].at[slot], relays[p].at[slot], recv1.at[p, slot]).wait()

    def forwards(n, wait):
        for p in range(3):
            owner = line_owner(p)
            here = (x, y, z)[p]
            sx, sy, sz = source_of(p, n, owner, here)
            mine = both_true(sx == x, sy == y, sz == z)
            copy = pass_on(p, n, n, owner, sx)
            aside, bypass = detour(p, n, owner, relays[p].at[n], send2.at[p, n])

            @pl.when(jnp.logical_not(mine))
            def _():
                if wait:
                    copy.wait_send()
                else:
                    arrived(p, n)

                    @pl.when(aside)
                    def _():
                        bypass.start()

                    @pl.when(jnp.logical_not(aside))
                    def _():
                        copy.start()

            slot = STEPS + n // 2
            fx, _, _ = source_of(p, n, owner, (owner[p] + 2) % 4)
            far = pass_on(p, n, slot, owner, fx)

            @pl.when(jnp.logical_and(here == beside(p, owner)[0], n % 2 == 1))
            def _():
                if wait:
                    far.wait_send()
                else:
                    arrived(p, slot)
                    far.start()

    repeat(STEPS, lambda n: sends(n, False))

    @pl.when(jnp.logical_not(is_owner))
    def _():
        repeat(STEPS, lambda n: forwards(n, False))
        repeat(STEPS, lambda n: forwards(n, True))

    def tile(half, s, r, slot):
        gram[slot] = lax.dot_general(
            xs[half, s], xs[core, r], (((1,), (1,)), ((), ())), preferred_element_type=jnp.float32
        )

    def half_tile(half, s, h, slot):
        lines = pl.ds(pl.multiple_of(h * 256, 256), 256)
        gram[slot, :, lines] = lax.dot_general(
            xs[half, s], xs[core, 3, lines], (((1,), (1,)), ((), ())), preferred_element_type=jnp.float32
        )

    def across(r):
        return pltpu.make_async_remote_copy(
            xs.at[core, r], xs.at[core, r], dsend.at[r], drecv.at[r], device_id=partner, device_id_type=MESH
        )

    def across_half(h):
        rows = xs.at[core, 3, pl.ds(pl.multiple_of(h * 256, 256), 256)]
        return pltpu.make_async_remote_copy(
            rows, rows, dsend.at[3 + h], drecv.at[3 + h], device_id=partner, device_id_type=MESH
        )

    def share_copy(m):
        return pltpu.make_async_remote_copy(
            final.at[m], landed.at[core], msend.at[m], mrecv.at[core], device_id=(m, klass), device_id_type=MESH
        )

    @pl.when(is_owner)
    def _():
        self_step = (4 - SKEW_Y) * x % 4 * 4 + (4 - SKEW_Z) * x % 4
        xs[core, self_step // 4, pl.ds(pl.multiple_of(self_step % 4 * 128 + x * UNIT, UNIT), UNIT)] = xs[
            other, 0, pl.ds(pl.multiple_of(klass * UNIT, UNIT), UNIT)
        ]
        repeat(STEPS, lambda n: sends(n, True))
        pl.semaphore_signal(credit, inc=1, device_id=partner, device_id_type=MESH)
        pl.semaphore_wait(credit, 1)
        pacc[...] = jnp.zeros_like(pacc)

        def take(half, r):
            pacc[...] += jnp.dot(pick_ref[half, r], xs[half, r], preferred_element_type=jnp.float32)

        def steps_in(r, first, count):
            for q in range(count):
                n = r * 4 + first + q
                for mine, count in ((False, 128), (True, 128 - UNIT)):
                    rows = xs.at[core, r, pl.ds(pl.multiple_of((first + q) * 128, 128), count)]

                    @pl.when((n == self_step) == mine)
                    def _():
                        pltpu.make_async_copy(rows, rows, rstep.at[n]).wait()

        def other_in(r):
            across(r).wait_recv()
            take(other, r)

            @pl.when(r % 2 == core)
            def _():
                tile(other, r, r, 16 + r // 2)

        def round_of(r):
            steps_in(r, 0, 4)
            across(r).start()
            take(core, r)

            def own_tile(s, carry):
                tile(core, s, r, r * (r + 1) // 2 + s)
                return carry

            lax.fori_loop(0, r + 1, own_tile, 0)

            @pl.when(r > 0)
            def _():
                other_in(r - 1)

            def cross_tile(s, carry):
                tile(other, s, r, 10 + r * (r - 1) // 2 + s)
                return carry

            lax.fori_loop(0, r, cross_tile, 0)

        repeat(3, round_of)

        def last_half(h):
            steps_in(3, 2 * h, 2)
            across_half(h).start()
            repeat(3, lambda s: half_tile(core, s, h, 6 + s))

            @pl.when(h == 0)
            def _():
                other_in(2)

            repeat(3, lambda s: half_tile(other, s, h, 13 + s))

        repeat(2, last_half)
        take(core, 3)
        tile(core, 3, 3, 9)
        for h in range(2):
            across_half(h).wait_recv()
        take(other, 3)

        @pl.when(core == 1)
        def _():
            tile(other, 3, 3, 17)

        wide = pacc[...]
        mass = wide[3:4]
        high = mass.astype(jnp.bfloat16).astype(jnp.float32)
        middle = (mass - high).astype(jnp.bfloat16).astype(jnp.float32)
        line = lax.broadcasted_iota(jnp.int32, (EXT, D), 0)
        hp = [0.5 * jnp.sum(wide[t : t + 1] * wide[t : t + 1], axis=1, keepdims=True) for t in range(3)]
        wide = jnp.where(line == 3, high, jnp.where(line == 4, middle, jnp.where(line == 5, mass - high - middle, wide)))
        picked = wide.astype(jnp.bfloat16)

        eye = lax.broadcasted_iota(jnp.int32, (128, 128), 0) == lax.broadcasted_iota(jnp.int32, (128, 128), 1)

        def group(n, xx):
            ny = (y + SKEW_Y * xx + n // 4) % 4
            nz = (z + SKEW_Z * xx + n % 4) % 4
            return ny, nz

        lane = lax.broadcasted_iota(jnp.int32, (8, 128), 1) // UNIT

        def own_rows(r):
            near = lax.dot_general(
                picked, xs[core, r], (((1,), (1,)), ((), ())), preferred_element_type=jnp.float32
            )
            for q in range(4):
                n = r * 4 + q
                lanes = slice(q * 128, q * 128 + 128)
                sub = gram[r * (r + 3) // 2, lanes, lanes]
                h = 0.5 * jnp.sum(jnp.where(eye, sub, 0.0), axis=0, keepdims=True)
                good = jnp.zeros((8, 128), jnp.float32)
                for xx in range(4):
                    ny, nz = group(n, xx)
                    piece = jnp.broadcast_to(valid_ref[core * 16 + xx * 4 + ny], (8, 128))
                    good = jnp.where(lane == xx, pltpu.roll(piece, (xx - nz + 4) % 4 * UNIT, 1), good)
                ok = good[0:1] > 0.0
                p1 = hp[0] - near[0:1, lanes]
                p2 = jnp.minimum(p1, hp[1] - near[1:2, lanes])
                p3 = jnp.minimum(p2, hp[2] - near[2:3, lanes])
                tab[core, r, 0:1, lanes] = jnp.where(ok, h, -BIG)
                tab[core, r, 1:2, lanes] = jnp.where(ok, p1, -BIG)
                tab[core, r, 2:3, lanes] = jnp.where(ok, p2, -BIG)
                tab[core, r, 3:4, lanes] = p3
                tab[core, r, 4:5, lanes] = h
                tab[core, r, 5:6, lanes] = good[0:1]
                tab[core, r, 6:7, lanes] = near[3:4, lanes] + near[4:5, lanes] + near[5:6, lanes]

        lax.fori_loop(0, 4, lambda r, carry: (own_rows(r), carry)[1], 0, unroll=4)
        sums[...] = jnp.zeros_like(sums)
        peak[...] = jnp.zeros_like(peak)
        tables = pltpu.make_async_remote_copy(
            tab.at[core], tab.at[core], tsend.at[0], trecv.at[0], device_id=partner, device_id_type=MESH
        )

        def row_block(b):
            half = jnp.where(b < 4, core, other)
            s = b % 4
            mine = b < 4

            @pl.when(b == 1)
            def _():
                tables.start()

            @pl.when(b == 4)
            def _():
                tables.wait()

            hcol[...] = column(tab[half, s, 0:1])
            a1col[...] = column(tab[half, s, 1:2])
            a2col[...] = column(tab[half, s, 2:3])
            r1[...] = jnp.zeros_like(r1)
            r2[...] = jnp.zeros_like(r2)

            def one_tile(r, carry):
                slot = jnp.where(
                    mine, r * (r + 1) // 2 + s, jnp.where(r == s, 16 + s // 2, 10 + r * (r - 1) // 2 + s)
                )
                diag = jnp.logical_and(mine, r == s)

                def sweep(rows_too):
                    for cb in range(4):
                        lanes = slice(cb * 128, cb * 128 + 128)
                        hu = tab[core, r, 0:1, lanes]
                        a1u = tab[core, r, 1:2, lanes]
                        a2u = tab[core, r, 2:3, lanes]

                        def strip(k, acc):
                            c1, c2, low = acc
                            at = pl.ds(pl.multiple_of(k * 32, 32), 32)
                            g = gram[slot, at, lanes]
                            e = g - hu
                            f = g - hcol[at]
                            c1 = c1 + fold(jnp.maximum(e + a1col[at], 0.0))
                            c2 = c2 + fold(jnp.maximum(e + a2col[at], 0.0))
                            low = jnp.minimum(
                                low, jnp.minimum(jnp.minimum(f[0:8], f[8:16]), jnp.minimum(f[16:24], f[24:32]))
                            )
                            if rows_too:
                                r1[at] += jnp.maximum(f + a1u, 0.0)
                                r2[at] += jnp.maximum(f + a2u, 0.0)
                            return c1, c2, low

                        zero = jnp.zeros((8, 128), jnp.float32)
                        c1, c2, low = lax.fori_loop(0, BS // 32, strip, (zero, zero, zero + BIG), unroll=16)
                        sums[r, 0, :, lanes] += c1
                        sums[r, 1, :, lanes] += c2
                        peak[...] = jnp.maximum(peak[...], hu - low)

                @pl.when(diag)
                def _():
                    sweep(False)

                @pl.when(jnp.logical_not(diag))
                def _():
                    sweep(True)

                return carry

            begin = jnp.where(jnp.logical_or(mine, s % 2 == core), s, s + 1)
            lax.fori_loop(begin, 4, one_tile, 0)
            for n, acc in enumerate((r1, r2)):
                part[half, s, n : n + 1] = jnp.sum(acc[...].T, axis=0, keepdims=True)

        repeat(8, row_block)
        best = jnp.max(jnp.max(peak[...], axis=0, keepdims=True), axis=1, keepdims=True)
        for r in range(4):
            part[other, r, 3:4] = jnp.broadcast_to(best, (1, BS))
        partial = pltpu.make_async_remote_copy(
            part.at[other], got, tsend.at[1], trecv.at[1], device_id=partner, device_id_type=MESH
        )
        total = jnp.sum(jnp.sum(valid_ref[...], axis=0), axis=1, keepdims=True)
        h_sum = jnp.zeros((1, 1), jnp.float32)
        for half in range(2):
            for r in range(4):
                h_sum = h_sum + jnp.sum(tab[half, r, 4:5], axis=1, keepdims=True)
        partial.start()
        partial.wait()
        bound = jnp.maximum(best, got[0, 3:4, 0:1]) * SCALE

        for r in range(4):
            cols = [jnp.sum(sums[r, n], axis=0, keepdims=True) + part[core, r, n : n + 1] + got[r, n : n + 1] for n in range(2)]
            h = tab[core, r, 4:5]
            ok = tab[core, r, 5:6] > 0.0
            far = total * h + h_sum - tab[core, r, 6:7]
            part[core, r, 4:5] = jnp.where(ok, (total * bound - far * SCALE) / total, 0.0)
            part[core, r, 5:6] = jnp.where(ok, cols[0] * SCALE / total, 0.0)
            part[core, r, 6:7] = jnp.where(ok, cols[1] * SCALE / total, 0.0)
            part[core, r, 7:8] = jnp.where(ok, jnp.maximum(bound - (h + tab[core, r, 3:4]) * SCALE, 0.0), 0.0)

        def natural(n):
            xx, ny = n // 4, n % 4
            i1 = (ny - y - SKEW_Y * xx + 16) % 4
            piece = jnp.zeros((8, 128), jnp.float32)
            for nz in range(4):
                i2 = (nz - z - SKEW_Z * xx + 16) % 4
                take = part[core, i1, :, pl.ds(pl.multiple_of(i2 * 128, 128), 128)]
                piece = jnp.where(lane == nz, pltpu.roll(take, (nz - xx + 4) % 4 * UNIT, 1), piece)
            seat = lax.broadcasted_iota(jnp.int32, (8, 128), 1) % UNIT // 4 == 2 * ny + core
            for m in range(8):
                spot = pltpu.roll(piece, (2 * ny + core - m + 32) * 4 % 128, 1)
                final[m, :, pl.ds(pl.multiple_of(xx * 128, 128), 128)] += jnp.where(seat, spot, 0.0)[4:8]

        final[...] = jnp.zeros_like(final)
        lax.fori_loop(0, 16, lambda n, carry: (natural(n), carry)[1], 0, unroll=8)
        me = lax.axis_index("dp")
        for m in range(8):
            local = jnp.logical_and(me == m, cls == klass)

            @pl.when(jnp.logical_not(local))
            def _():
                share_copy(m).start()

            @pl.when(local)
            def _():
                landed[core] = final[m]

        for m in range(8):
            local = jnp.logical_and(me == m, cls == klass)

            @pl.when(jnp.logical_not(local))
            def _():
                share_copy(m).wait_send()

        repeat(3, lambda r: across(r).wait_send())
        repeat(2, lambda h: across_half(h).wait_send())

    @pl.when(jnp.logical_not(is_owner))
    def _():
        repeat(STEPS, lambda n: sends(n, True))

    for c in range(2):
        local = both_true(is_owner, core == c, cls == klass)

        @pl.when(jnp.logical_not(local))
        def _():
            pltpu.make_async_copy(landed.at[c], landed.at[c], mrecv.at[c]).wait()


def select_facilities(target, sketches, pick, valid):
    vmem = pl.BlockSpec(memory_space=pltpu.VMEM)
    sems = pltpu.SemaphoreType.DMA
    wide = pltpu.VMEM((BS, 128), jnp.float32)
    return pl.pallas_call(
        kernel,
        out_shape=jax.ShapeDtypeStruct((2, 4, BS), jnp.float32),
        in_specs=[vmem, pl.BlockSpec(memory_space=pl.ANY), vmem, vmem],
        out_specs=vmem,
        scratch_shapes=[pltpu.VMEM((2, 4, BS, D), jnp.bfloat16)]
        + [pltpu.VMEM((STEPS + STEPS // 2, UNIT, size), jnp.bfloat16) for _, size in PARTS]
        + [
            pltpu.VMEM((18, BS, BS), jnp.float32),
            pltpu.VMEM((2, 4, 8, BS), jnp.float32),
            wide, wide, wide, wide, wide,
            pltpu.VMEM((4, 2, 8, BS), jnp.float32),
            pltpu.VMEM((8, 128), jnp.float32),
            pltpu.VMEM((2, 4, 8, BS), jnp.float32),
            pltpu.VMEM((4, 8, BS), jnp.float32),
            pltpu.VMEM((8, 4, BS), jnp.float32),
            pltpu.VMEM((EXT, D), jnp.float32),
            sems((3, STEPS)), sems((3, STEPS + STEPS // 2)), sems((3, STEPS + STEPS // 2)), sems((STEPS,)),
            sems((5,)), sems((5,)), sems((2,)), sems((2,)), sems((8,)), sems((2,)),
            sems, pltpu.SemaphoreType.REGULAR,
        ],
        compiler_params=pltpu.CompilerParams(collective_id=0, has_side_effects=True, vmem_limit_bytes=62 * 1024 * 1024),
        name="facilities",
    )(target, sketches, pick, valid)


def body(sketches, labels, places, counts, chosen):
    member = lax.axis_index("dp")
    cls = lax.axis_index("cls")
    pairs = [(n, n ^ 1) for n in range(16)]
    counts_there = lax.ppermute(counts, "cls", pairs)
    chosen_there = lax.ppermute(chosen, "cls", pairs)
    target = labels * UNIT + places // 512 * 4 + places % 4

    x, y, z, core = member // 2, (cls // 2) % 4, (member % 2) * 2 + cls // 8, cls % 2
    ours = core == z // 2
    picked = jnp.where(ours, chosen, chosen_there)[:, 0]
    class_counts = jnp.where(ours, counts, counts_there)[0]
    source = picked % 512 // 4
    sx, sz, sy, score = source // 32, source // 8 % 4, source // 2 % 4, source % 2
    step = (sy - y - SKEW_Y * sx + 16) % 4 * 4 + (sz - z - SKEW_Z * sx + 16) % 4
    where = score * HALF + step * 128 + sx * UNIT + picked // 512 * 4 + picked % 4
    spot = jnp.pad(where, (0, EXT - 3), constant_values=-1)
    line = jnp.arange(4096, dtype=jnp.int32).reshape(8, 1, BS)
    everyone = jnp.arange(EXT, dtype=jnp.int32)[None, :, None] == 3
    pick = ((line == spot[None, :, None]) | everyone).astype(jnp.bfloat16).reshape(2, 4, EXT, BS)
    by_source = jnp.transpose(class_counts.reshape(8, 4, 4, 4, 2), (4, 1, 3, 2, 0))
    valid = (jnp.arange(4, dtype=jnp.int32) < by_source[..., None]).astype(jnp.float32).reshape(32, 1, 128)

    both = select_facilities(target[None, :], sketches, pick, valid)
    return (both[0, :3, None, :] + both[1, :3, None, :], both[0, 3:] + both[1, 3:])


def solution(mesh):
    placed = (
        P(("dp", "cls"), None),
        P(("dp", "cls")),
        P(("dp", "cls")),
        P("cls", None, None),
        P(None, "cls"),
    )
    return jax.shard_map(
        body,
        mesh=mesh,
        in_specs=placed,
        out_specs=(P(None, "cls", "dp"), P("cls", "dp")),
        check_vma=False,
    )
```
